128 devices in a mesh: gx: 16 (over y, z), gy: 8 (over x, core).
Axes of the slice: x: 4, y: 4, z: 4, core: 2. Of those that a mesh axis runs over, the one named last changes fastest.
Arguments:
- state: float32 [4, 5, 5, 128, 2048], P(None, None, None, 'gy', 'gx'), may hold values from -3 to 60, as said below
Outputs:
- advanced: float32 [4, 5, 5, 128, 2048], P(None, None, None, 'gy', 'gx')
- tendency: float32 [4, 5, 5, 128, 2048], P(None, None, None, 'gy', 'gx')
The draws below stay inside these ranges and needn't reach their ends.
Inputs may be any that keep to these rules, and one draw needn't show every extreme that they name: `state`: at every node density is at least 0.2 and pressure, 0.4 times (energy minus half the squared momentum over density), is at least 0.2.
All inputs are finite; a program needn't handle non-finite values.
Results may differ from the reference program's by a relative error of at most 0.0003.
Values sent between devices are 32-bit elements; how exact they have to be, the bound alone decides.
No kernel may reach another device: no remote copies, remote signals or barrier semaphores. Data moves between devices by JAX's collectives and lax.ppermute only.
A program may use at most 128 MiB of HBM per device.

```python
import math
import jax
import jax.numpy as jnp
import numpy as np
from jax import lax

NR = 128
NC = 2048


def draw_state(key, part):
    subkeys = jax.random.split(key, 6)
    column = jnp.arange(NC, dtype=jnp.float32)
    profile = 5.0 - 4.0 * jnp.cos(2.0 * math.pi * column / NC)
    shape_elem = (NR, NC)
    density = jax.random.uniform(subkeys[0], shape_elem, jnp.float32, 0.5, 1.5)
    pressure = profile * jax.random.uniform(subkeys[1], shape_elem, jnp.float32, 0.6, 1.4)
    jitter = jnp.clip(jax.random.normal(subkeys[2], (4, 5, 5, NR, NC), jnp.float32), -2.5, 2.5)
    drift_first = jax.random.uniform(subkeys[3], shape_elem, jnp.float32, -0.5, 0.5)
    drift_second = jax.random.uniform(subkeys[4], shape_elem, jnp.float32, -0.5, 0.5)
    amplitude = jnp.exp(jax.random.uniform(subkeys[5], shape_elem, jnp.float32, math.log(0.001), math.log(0.2)))
    node_density = density * (1.0 + amplitude * jitter[0])
    node_pressure = pressure * (1.0 + amplitude * jitter[3])
    node_first = drift_first + 0.5 * amplitude * jitter[1]
    node_second = drift_second + 0.5 * amplitude * jitter[2]
    energy = node_pressure / 0.4 + 0.5 * node_density * (node_first * node_first + node_second * node_second)
    return jnp.stack([node_density, node_density * node_first, node_density * node_second, energy]).astype(jnp.float32)


def setup_inputs(seed: int = 0) -> dict:
    streams_of = jax.random.split(jax.random.key(seed), 2)
    state = draw_state(jax.random.fold_in(streams_of[1], 71), 0)
    return {"state": state}


ADIABATIC = 1.4
COURANT = 0.2
ALPHA_MAX = 0.5

def tables():
    lobatto = np.array([-1.0, -math.sqrt(3.0 / 7.0), 0.0, math.sqrt(3.0 / 7.0), 1.0])
    weights = np.array([0.1, 49.0 / 90.0, 32.0 / 45.0, 49.0 / 90.0, 0.1])
    identity = np.eye(5)
    distance = lobatto[:, None] - lobatto[None, :] + identity
    barycentric = 1.0 / np.prod(distance, axis=1)
    derivative = (1.0 - identity) * (barycentric[None, :] / barycentric[:, None]) / distance
    derivative = derivative - identity * derivative.sum(axis=1)[:, None]
    legendre = np.zeros((5, 5))
    legendre[:, 0] = 1.0
    legendre[:, 1] = lobatto
    for degree in range(2, 5):
        legendre[:, degree] = ((2 * degree - 1) * lobatto * legendre[:, degree - 1] - (degree - 1) * legendre[:, degree - 2]) / degree
    norms = np.array([2.0, 2.0 / 3.0, 2.0 / 5.0, 2.0 / 7.0, 0.5])
    inverse = (legendre * weights[:, None]).T / norms[:, None]
    levels = np.maximum(np.arange(5)[:, None], np.arange(5)[None, :])
    return (jnp.asarray(derivative, jnp.float32), jnp.asarray(weights, jnp.float32), jnp.asarray(inverse, jnp.float32), jnp.asarray(levels == 4, jnp.float32), jnp.asarray(levels == 3, jnp.float32), jnp.asarray(levels <= 3, jnp.float32))

def slice_of(source, along_dim, begin_at, end_at):
    return lax.slice_in_dim(source, begin_at, end_at, axis=along_dim)

def slice_all(fields, along_dim, begin_at, end_at):
    return tuple((slice_of(member, along_dim, begin_at, end_at) for member in fields))

def primitive(conserved):
    density = conserved[0]
    speed_first = conserved[1] / density
    speed_second = conserved[2] / density
    pressure = (ADIABATIC - 1.0) * (conserved[3] - 0.5 * density * (speed_first * speed_first + speed_second * speed_second))
    return (density, speed_first, speed_second, pressure)

def log_mean(left_val, right_val):
    relative = (left_val * (left_val - 2.0 * right_val) + right_val * right_val) / (left_val * (left_val + 2.0 * right_val) + right_val * right_val)
    nearby = relative < 0.0001
    series = (left_val + right_val) * 52.5 / (105.0 + relative * (35.0 + relative * (21.0 + relative * 15.0)))
    logged = jnp.where(nearby, 1.0, jnp.log(right_val / left_val))
    return jnp.where(nearby, series, (right_val - left_val) / logged)

def two_point(left_state, right_state, normal_dir):
    mean_density = log_mean(left_state[0], right_state[0])
    thermal_mean = left_state[3] * right_state[3] / log_mean(left_state[0] * right_state[3], right_state[0] * left_state[3])
    mean_first = 0.5 * (left_state[1] + right_state[1])
    mean_second = 0.5 * (left_state[2] + right_state[2])
    mean_pressure = 0.5 * (left_state[3] + right_state[3])
    square_mean = 0.5 * (left_state[1] * right_state[1] + left_state[2] * right_state[2])
    left_normal = left_state[1 + normal_dir]
    right_normal = right_state[1 + normal_dir]
    mass_flux = mean_density * 0.5 * (left_normal + right_normal)
    push_first = mass_flux * mean_first + (mean_pressure if normal_dir == 0 else 0.0)
    push_second = mass_flux * mean_second + (mean_pressure if normal_dir == 1 else 0.0)
    energy_flux = mass_flux * (square_mean + thermal_mean / (ADIABATIC - 1.0)) + 0.5 * (left_state[3] * right_normal + right_state[3] * left_normal)
    return jnp.stack(jnp.broadcast_arrays(mass_flux, push_first, push_second, energy_flux))

def physical(primitives, normal_dir):
    normal_speed = primitives[1 + normal_dir]
    mass_flux = primitives[0] * normal_speed
    energy = primitives[3] / (ADIABATIC - 1.0) + 0.5 * primitives[0] * (primitives[1] * primitives[1] + primitives[2] * primitives[2])
    push_first = mass_flux * primitives[1] + (primitives[3] if normal_dir == 0 else 0.0)
    push_second = mass_flux * primitives[2] + (primitives[3] if normal_dir == 1 else 0.0)
    return jnp.stack([mass_flux, push_first, push_second, normal_speed * (energy + primitives[3])])

def wave(primitives, normal_dir):
    return jnp.abs(primitives[1 + normal_dir]) + jnp.sqrt(ADIABATIC * primitives[3] / primitives[0])

def direction_terms(conserved, primitives, normal_dir, derivative, weights):
    node_dim = 1 if normal_dir == 0 else 0
    elem_dim = 3 if normal_dir == 0 else 2
    flux_dim = node_dim + 1
    element_count = primitives[0].shape[elem_dim]
    shaper = [1, 1, 1, 1, 1]
    shaper[flux_dim] = 5
    volume = jnp.zeros(conserved.shape, jnp.float32)
    for partner in range(5):
        pair_flux = two_point(primitives, slice_all(primitives, node_dim, partner, partner + 1), normal_dir)
        volume = volume + (2.0 * derivative[:, partner]).reshape(tuple(shaper)) * pair_flux
    upper_trace = slice_all(primitives, node_dim, 4, 5)
    lower_trace = slice_all(primitives, node_dim, 0, 1)
    inner_left = slice_all(upper_trace, elem_dim, 0, element_count - 1)
    inner_right = slice_all(lower_trace, elem_dim, 1, element_count)
    state_left = slice_of(slice_of(conserved, flux_dim, 4, 5), elem_dim + 1, 0, element_count - 1)
    state_right = slice_of(slice_of(conserved, flux_dim, 0, 1), elem_dim + 1, 1, element_count)
    fastest = jnp.maximum(wave(inner_left, normal_dir), wave(inner_right, normal_dir))
    face_flux = two_point(inner_left, inner_right, normal_dir) - 0.5 * fastest * (state_right - state_left)
    flux_before = slice_of(face_flux, elem_dim + 1, 0, element_count - 2)
    flux_after = slice_of(face_flux, elem_dim + 1, 1, element_count - 1)
    inside = slice_all(primitives, elem_dim, 1, element_count - 1)
    inside_state = slice_of(conserved, elem_dim + 1, 1, element_count - 1)
    own_flux = physical(inside, normal_dir)
    volume = slice_of(volume, elem_dim + 1, 1, element_count - 1)
    middle = jnp.zeros_like(slice_of(own_flux, flux_dim, 0, 3))
    surface = jnp.concatenate([-(flux_before - slice_of(own_flux, flux_dim, 0, 1)) / weights[0], middle, (flux_after - slice_of(own_flux, flux_dim, 4, 5)) / weights[4]], axis=flux_dim)
    high_order = -(volume + surface)
    spread = jnp.maximum(wave(slice_all(inside, node_dim, 0, 4), normal_dir), wave(slice_all(inside, node_dim, 1, 5), normal_dir))
    subcell = 0.5 * (slice_of(own_flux, flux_dim, 0, 4) + slice_of(own_flux, flux_dim, 1, 5)) - 0.5 * spread * (slice_of(inside_state, flux_dim, 1, 5) - slice_of(inside_state, flux_dim, 0, 4))
    wall_flux = jnp.concatenate([flux_before, subcell, flux_after], axis=flux_dim)
    weight_column = weights.reshape(tuple(shaper))
    low_order = -(slice_of(wall_flux, flux_dim, 1, 6) - slice_of(wall_flux, flux_dim, 0, 5)) / weight_column
    return (high_order, low_order)

def blending(primitives, inverse, top_mask, next_mask, lower_mask):
    indicator = primitives[0] * primitives[3]
    modal_coef = jnp.einsum('ka,lb,abrc->klrc', inverse, inverse, indicator, precision=lax.Precision.HIGHEST)
    squares = modal_coef * modal_coef
    total_energy = lax.optimization_barrier(jnp.sum(squares, axis=(0, 1)))
    top_part = lax.optimization_barrier(jnp.sum(squares * top_mask[:, :, None, None], axis=(0, 1)))
    next_part = lax.optimization_barrier(jnp.sum(squares * next_mask[:, :, None, None], axis=(0, 1)))
    lower_part = lax.optimization_barrier(jnp.sum(squares * lower_mask[:, :, None, None], axis=(0, 1)))
    energy = jnp.maximum(top_part / total_energy, next_part / lower_part)
    threshold = 0.5 * 10.0 ** (-1.8 * 5.0 ** 0.25)
    sharpness = math.log((1.0 - 0.0001) / 0.0001)
    sigmoid_val = 1.0 / (1.0 + jnp.exp(-sharpness / threshold * (energy - threshold)))
    capped = jnp.minimum(sigmoid_val, ALPHA_MAX)
    centre = capped[1:-1, 1:-1]
    beside_all = jnp.maximum(jnp.maximum(capped[:-2, 1:-1], capped[2:, 1:-1]), jnp.maximum(capped[1:-1, :-2], capped[1:-1, 2:]))
    return jnp.maximum(centre, 0.5 * beside_all)

def tendency_of(conserved, table_set):
    derivative, weights, inverse, top_mask, next_mask, lower_mask = table_set
    primitives = primitive(conserved)
    high_columns, low_columns = direction_terms(conserved, primitives, 0, derivative, weights)
    high_rows, low_rows = direction_terms(conserved, primitives, 1, derivative, weights)
    blend_factor = blending(primitives, inverse, top_mask, next_mask, lower_mask)
    high_order = high_columns[:, :, :, 1:-1, :] + high_rows[:, :, :, :, 1:-1]
    low_order = low_columns[:, :, :, 1:-1, :] + low_rows[:, :, :, :, 1:-1]
    return (1.0 - blend_factor) * high_order + blend_factor * low_order

def full_tendency(conserved, table_set):
    padded = jnp.pad(conserved, ((0, 0), (0, 0), (0, 0), (1, 1), (1, 1)), mode='wrap')
    row_count = conserved.shape[3]
    block_rows = 16 if row_count % 16 == 0 else row_count

    def one_block(block_index):
        window = lax.dynamic_slice_in_dim(padded, block_index * block_rows, block_rows + 2, axis=3)
        return tendency_of(window, table_set)
    pieces = lax.map(one_block, jnp.arange(row_count // block_rows, dtype=jnp.int32))
    return jnp.moveaxis(pieces, 0, 3).reshape(conserved.shape)

def reference(state):
    table_set = tables()
    primitives = primitive(state)
    fastest = jnp.max(jnp.sqrt(primitives[1] * primitives[1] + primitives[2] * primitives[2]) + jnp.sqrt(ADIABATIC * primitives[3] / primitives[0]))
    delta_time = COURANT * 2.0 / (9.0 * fastest)
    rate_first = full_tendency(state, table_set)
    first_state = state + delta_time * rate_first
    rate_second = full_tendency(first_state, table_set)
    advanced = 0.5 * state + 0.5 * (first_state + delta_time * rate_second)
    return (advanced, rate_second)
```

```python
import math

import jax
import jax.numpy as jnp
import numpy as np
from jax import lax
from jax.experimental import pallas as pl
from jax.experimental.pallas import tpu as pltpu
from jax.sharding import Mesh
from jax.sharding import PartitionSpec as P

GX = ("gx_0", "gx_1")
GY = ("gy_0", "gy_1")
ALL = ("gx_0", "gx_1", "gy_0", "gy_1")


ADIABATIC = 1.4
COURANT = 0.2
ALPHA_MAX = 0.5
ROWS = 16
COLS = 128
F32 = jnp.float32


def tables():
    lobatto = np.array([-1.0, -math.sqrt(3.0 / 7.0), 0.0, math.sqrt(3.0 / 7.0), 1.0])
    weights = np.array([0.1, 49.0 / 90.0, 32.0 / 45.0, 49.0 / 90.0, 0.1])
    identity = np.eye(5)
    distance = lobatto[:, None] - lobatto[None, :] + identity
    barycentric = 1.0 / np.prod(distance, axis=1)
    derivative = (1.0 - identity) * (barycentric[None, :] / barycentric[:, None]) / distance
    derivative = derivative - identity * derivative.sum(axis=1)[:, None]
    legendre = np.zeros((5, 5))
    legendre[:, 0] = 1.0
    legendre[:, 1] = lobatto
    for degree in range(2, 5):
        legendre[:, degree] = (
            (2 * degree - 1) * lobatto * legendre[:, degree - 1]
            - (degree - 1) * legendre[:, degree - 2]
        ) / degree
    norms = np.array([2.0, 2.0 / 3.0, 2.0 / 5.0, 2.0 / 7.0, 0.5])
    inverse = (legendre * weights[:, None]).T / norms[:, None]
    return derivative, weights, inverse


DERIVATIVE, WEIGHTS, INVERSE = tables()
SKEW = WEIGHTS[:, None] * DERIVATIVE
PER_WEIGHT = 1.0 / WEIGHTS
SCALE = (1.0, 0.5, 0.5, 0.5)
LN2 = math.log(2.0)


def node_values(rho, mx, my, en):
    inv_rho = 1.0 / rho
    vx = mx * inv_rho
    vy = my * inv_rho
    pressure = 0.4 * (en - 0.5 * (mx * vx + my * vy))
    return vx, vy, pressure, inv_rho


def thermal(rho, pressure, inv_rho):
    beta = rho * (1.0 / pressure)
    theta = pressure * inv_rho
    return beta, theta


class Node:
    def __init__(self, rho, vn, vt, p, beta, inv_rho, theta):
        self.rho, self.vn, self.vt, self.p = rho, vn, vt, p
        self.beta, self.inv_rho, self.theta = beta, inv_rho, theta


def pair(left, right, q):
    s = left.rho + right.rho
    d = right.rho - left.rho
    near = jnp.abs(d) < 0.01 * s
    logged = 0.5 * jnp.log(right.rho * left.inv_rho)
    t = d * (1.0 / jnp.where(near, s, logged))
    f = t * t
    series = 1.0 + f * (1.0 / 3.0 + f * (0.2 + f * (1.0 / 7.0)))
    mean2 = jnp.where(near, s * (1.0 / series), t)
    sb = left.beta + right.beta
    db = right.beta - left.beta
    nearb = jnp.abs(db) < 0.01 * sb
    loggedb = 5.0 * jnp.log(right.beta * left.theta)
    r = 1.0 / jnp.where(nearb, sb, db)
    tb = db * r
    fb = tb * tb
    seriesb = 10.0 + fb * (10.0 / 3.0 + fb * (2.0 + fb * (10.0 / 7.0)))
    warm = jnp.where(nearb, seriesb, loggedb) * r
    vn = left.vn + right.vn
    vt = left.vt + right.vt
    ps = left.p + right.p
    mass = (mean2 * vn) * (0.5 * q)
    along = mass * vn + ps * (2.0 * q)
    across = mass * vt
    dot = left.vn * right.vn + left.vt * right.vt
    energy = mass * (dot + warm) + (left.p * right.vn + right.p * left.vn) * (2.0 * q)
    return mass, along, across, energy


def line_terms(nodes, cons, speeds):
    high = [[None] * 5 for _ in range(4)]
    for i in range(5):
        for j in range(i + 1, 5):
            flux = pair(nodes[i], nodes[j], float(SKEW[i, j]))
            for v in range(4):
                high[v][i] = flux[v] if high[v][i] is None else high[v][i] + flux[v]
                high[v][j] = -flux[v] if high[v][j] is None else high[v][j] - flux[v]
    own = []
    for node, (rho, mn, mt, en) in zip(nodes, cons):
        own.append((mn, mn * node.vn + node.p, mn * node.vt, node.vn * (en + node.p)))
    less = [[None] * 5 for _ in range(4)]
    for v in range(4):
        before = None
        for i in range(4):
            spread = jnp.maximum(speeds[i], speeds[i + 1])
            inner = own[i][v] + own[i + 1][v] - spread * (cons[i + 1][v] - cons[i][v])
            if v == 0:
                inner = 0.5 * inner
            here = inner if before is None else inner - before
            less[v][i] = here - high[v][i]
            before = inner
        less[v][4] = -before - high[v][4]
    return high, less


def sound(theta):
    return jnp.sqrt(ADIABATIC * theta)


def face(left_cons, right_cons, normal):
    sides = []
    speeds = []
    for rho, mx, my, en in (left_cons, right_cons):
        vx, vy, p, inv_rho = node_values(rho, mx, my, en)
        beta, theta = thermal(rho, p, inv_rho)
        vn, vt = (vx, vy) if normal == 0 else (vy, vx)
        sides.append(Node(rho, vn, vt, p, beta, inv_rho, theta))
        speeds.append(jnp.abs(vn) + sound(theta))
    mass, along, across, energy = pair(sides[0], sides[1], 0.5)
    flux = (mass, along, across, energy) if normal == 0 else (mass, across, along, energy)
    fastest = jnp.maximum(speeds[0], speeds[1])
    out = []
    for v in range(4):
        jump = fastest * (right_cons[v] - left_cons[v])
        out.append(flux[v] - (0.5 * jump if v == 0 else jump))
    return out


def transform(values):
    s0, s1 = values[0] + values[4], values[1] + values[3]
    d0, d1 = values[0] - values[4], values[1] - values[3]
    out = []
    for k in range(5):
        c = [float(x) for x in INVERSE[k]]
        if k % 2 == 0:
            out.append(c[0] * s0 + c[1] * s1 + c[2] * values[2])
        else:
            out.append(c[0] * d0 + c[1] * d1)
    return out


def raw_indicator(indicator):
    along = [transform(indicator[a]) for a in range(5)]
    modal = [transform([along[a][l] for a in range(5)]) for l in range(5)]
    levels = [None] * 5
    for l in range(5):
        for k in range(5):
            square = modal[l][k] * modal[l][k]
            level = max(k, l)
            levels[level] = square if levels[level] is None else levels[level] + square
    lower = levels[0] + levels[1] + levels[2] + levels[3]
    total = lower + levels[4]
    energy = jnp.maximum(levels[4] / total, levels[3] / lower)
    threshold = 0.5 * 10.0 ** (-1.8 * 5.0**0.25)
    sharpness = math.log((1.0 - 0.0001) / 0.0001)
    sigmoid = 1.0 / (1.0 + jnp.exp(-sharpness / threshold * (energy - threshold)))
    return jnp.minimum(sigmoid, ALPHA_MAX)


def lanes():
    return lax.broadcasted_iota(jnp.int32, (8, COLS), 1)


def sublanes():
    return lax.broadcasted_iota(jnp.int32, (8, COLS), 0)


def pack_borders(get, raws, cols_ref, up_ref, down_ref):
    lane = lanes()
    for i in range(2):
        packed = jnp.zeros((8, COLS), F32)
        for v in range(4):
            for a in range(5):
                j = v * 5 + a
                first = get(v, a, 0, pl.ds(8 * i, 8))
                last = get(v, a, 4, pl.ds(8 * i, 8))
                packed = jnp.where(lane == j, first if j == 0 else pltpu.roll(first, j, 1), packed)
                packed = jnp.where(lane == 64 + j, pltpu.roll(last, 65 + j, 1), packed)
        packed = jnp.where(lane == 20, pltpu.roll(raws[i], 20, 1), packed)
        packed = jnp.where(lane == 84, pltpu.roll(raws[i], 85, 1), packed)
        cols_ref[pl.ds(8 * i, 8), :] = packed
    for v in range(4):
        for b in range(5):
            j = v * 5 + b
            up_ref[j : j + 1, :] = get(v, 4, b, pl.ds(15, 1))
            down_ref[j : j + 1, :] = get(v, 0, b, pl.ds(0, 1))
    up_ref[20:21, :] = raws[1][7:8, :]
    down_ref[20:21, :] = raws[0][0:1, :]
    zeros = jnp.zeros((3, COLS), F32)
    up_ref[21:24, :] = zeros
    down_ref[21:24, :] = zeros


def start_kernel(u_ref, top_ref, raw_ref, cols_ref, up_ref, down_ref):
    raws = []
    top = None
    for i in range(2):
        rows = pl.ds(8 * i, 8)
        indicator = [[None] * 5 for _ in range(5)]
        for a in range(5):
            for b in range(5):
                rho, mx, my, en = (u_ref[v, a, b, rows, :] for v in range(4))
                vx, vy, p, inv_rho = node_values(rho, mx, my, en)
                indicator[a][b] = rho * p
                speed = jnp.sqrt(vx * vx + vy * vy) + sound(p * inv_rho)
                top = speed if top is None else jnp.maximum(top, speed)
        raws.append(raw_indicator(indicator))
        raw_ref[rows, :] = raws[i]
    top_ref[...] = jnp.broadcast_to(jnp.max(top).reshape(1, 1, 1), top_ref.shape)
    pack_borders(lambda v, a, b, rows: u_ref[v, a, b, rows, :], raws, cols_ref, up_ref, down_ref)


def volume_kernel(u_ref, high_ref, less_ref, work_ref):
    def chunk(i, carry):
        rows = pl.ds(pl.multiple_of(8 * i, 8), 8)
        for a in range(5):
            for b in range(5):
                rho, mx, my, en = (u_ref[v, a, b, rows, :] for v in range(4))
                vx, vy, p, inv_rho = node_values(rho, mx, my, en)
                beta, theta = thermal(rho, p, inv_rho)
                for k, x in enumerate((vx, vy, p, beta, inv_rho, theta, sound(theta))):
                    work_ref[k, a, b] = x
        for normal in range(2):
            for across in range(5):
                nodes, cons, speeds = [], [], []
                for along in range(5):
                    a, b = (across, along) if normal == 0 else (along, across)
                    rho, mx, my, en = (u_ref[v, a, b, rows, :] for v in range(4))
                    vx, vy, p, beta, inv_rho, theta, c = (work_ref[k, a, b] for k in range(7))
                    vn, vt, mn, mt = (vx, vy, mx, my) if normal == 0 else (vy, vx, my, mx)
                    nodes.append(Node(rho, vn, vt, p, beta, inv_rho, theta))
                    cons.append((rho, mn, mt, en))
                    speeds.append(jnp.abs(vn) + c)
                high, less = line_terms(nodes, cons, speeds)
                for along in range(5):
                    a, b = (across, along) if normal == 0 else (along, across)
                    for k in range(4):
                        v = k if normal == 0 else (0, 2, 1, 3)[k]
                        scale = -float(PER_WEIGHT[along]) * SCALE[v]
                        if normal == 0:
                            high_ref[v, a, b, rows, :] = scale * high[k][along]
                            less_ref[v, a, b, rows, :] = scale * less[k][along]
                        else:
                            high_ref[v, a, b, rows, :] += scale * high[k][along]
                            less_ref[v, a, b, rows, :] += scale * less[k][along]
        return carry

    lax.fori_loop(0, 2, chunk, 0)


def rates(i, get, high_ref, less_ref, raw_ref, halo_refs, emit):
    left_ref, right_ref, below_ref, above_ref = halo_refs
    rows = pl.ds(8 * i, 8)
    lane, sublane = lanes(), sublanes()
    from_left = left_ref[rows, :]
    from_right = right_ref[rows, :]

    def from_before_x(x, j):
        return jnp.where(lane == 0, pltpu.roll(from_left, (128 - 64 - j) % 128, 1), pltpu.roll(x, 1, 1))

    def from_after_x(x, j):
        return jnp.where(lane == 127, pltpu.roll(from_right, 127 - j, 1), pltpu.roll(x, 127, 1))

    def from_before_y(x, other):
        return jnp.where(sublane == 0, jnp.broadcast_to(other, (8, COLS)), pltpu.roll(x, 1, 0))

    def from_after_y(x, other):
        return jnp.where(sublane == 7, jnp.broadcast_to(other, (8, COLS)), pltpu.roll(x, 7, 0))

    capped = raw_ref[rows, :]
    below = from_before_y(capped, below_ref[20:21, :] if i == 0 else raw_ref[7:8, :])
    above = from_after_y(capped, above_ref[20:21, :] if i == 1 else raw_ref[8:9, :])
    beside = jnp.maximum(
        jnp.maximum(below, above),
        jnp.maximum(from_before_x(capped, 20), from_after_x(capped, 20)),
    )
    blend = jnp.maximum(capped, 0.5 * beside)

    ends = {}
    for a in range(5):
        lower = [get(v, a, 0, rows) for v in range(4)]
        upper = [get(v, a, 4, rows) for v in range(4)]
        before = [from_before_x(upper[v], v * 5 + a) for v in range(4)]
        after = [from_after_x(lower[v], v * 5 + a) for v in range(4)]
        for b, flux, sign in (
            (0, face(before, lower, 0), 1.0),
            (4, face(upper, after, 0), -1.0),
        ):
            for v in range(4):
                ends[v, a, b] = (sign * float(PER_WEIGHT[b]) * SCALE[v]) * flux[v]
    for b in range(5):
        lower = [get(v, 0, b, rows) for v in range(4)]
        upper = [get(v, 4, b, rows) for v in range(4)]
        before, after = [], []
        for v in range(4):
            j = v * 5 + b
            other = below_ref[j : j + 1, :] if i == 0 else get(v, 4, b, pl.ds(7, 1))
            before.append(from_before_y(upper[v], other))
            other = above_ref[j : j + 1, :] if i == 1 else get(v, 0, b, pl.ds(8, 1))
            after.append(from_after_y(lower[v], other))
        for a, flux, sign in (
            (0, face(before, lower, 1), 1.0),
            (4, face(upper, after, 1), -1.0),
        ):
            for v in range(4):
                term = (sign * float(PER_WEIGHT[a]) * SCALE[v]) * flux[v]
                ends[v, a, b] = ends[v, a, b] + term if (v, a, b) in ends else term
    for a in range(5):
        for b in range(5):
            for v in range(4):
                rate = high_ref[v, a, b, rows, :] + blend * less_ref[v, a, b, rows, :]
                if (v, a, b) in ends:
                    rate = rate + ends[v, a, b]
                emit(v, a, b, rows, rate)


def step_of(tops_ref):
    top = tops_ref[0]
    for k in range(1, 128):
        top = jnp.maximum(top, tops_ref[k])
    return (COURANT * 2.0 / 9.0) / jnp.broadcast_to(top, (8, COLS))


def first_kernel(
    tops_ref, u_ref, high_ref, less_ref, raw_ref, left_ref, right_ref, below_ref, above_ref,
    first_ref, next_raw_ref, cols_ref, up_ref, down_ref,
):
    step = step_of(tops_ref)
    halos = (left_ref, right_ref, below_ref, above_ref)

    def get(v, a, b, rows):
        return u_ref[v, a, b, rows, :]

    def emit(v, a, b, rows, rate):
        first_ref[v, a, b, rows, :] = u_ref[v, a, b, rows, :] + step * rate

    raws = []
    for i in range(2):
        rates(i, get, high_ref, less_ref, raw_ref, halos, emit)
        rows = pl.ds(8 * i, 8)
        indicator = [[None] * 5 for _ in range(5)]
        for a in range(5):
            for b in range(5):
                rho, mx, my, en = (first_ref[v, a, b, rows, :] for v in range(4))
                indicator[a][b] = rho * node_values(rho, mx, my, en)[2]
        raws.append(raw_indicator(indicator))
        next_raw_ref[rows, :] = raws[i]
    pack_borders(
        lambda v, a, b, rows: first_ref[v, a, b, rows, :], raws, cols_ref, up_ref, down_ref
    )


def last_kernel(
    tops_ref, u_ref, first_ref, high_ref, less_ref, raw_ref, left_ref, right_ref, below_ref, above_ref,
    advanced_ref, tendency_ref,
):
    step = step_of(tops_ref)
    halos = (left_ref, right_ref, below_ref, above_ref)

    def get(v, a, b, rows):
        return first_ref[v, a, b, rows, :]

    def emit(v, a, b, rows, rate):
        tendency_ref[v, a, b, rows, :] = rate
        first = first_ref[v, a, b, rows, :] + step * rate
        advanced_ref[v, a, b, rows, :] = 0.5 * (u_ref[v, a, b, rows, :] + first)

    for i in range(2):
        rates(i, get, high_ref, less_ref, raw_ref, halos, emit)


FIELD = jax.ShapeDtypeStruct((4, 5, 5, ROWS, COLS), F32)
RAW = jax.ShapeDtypeStruct((ROWS, COLS), F32)
ROW = jax.ShapeDtypeStruct((24, COLS), F32)
TOPS = jax.ShapeDtypeStruct((128, 1, COLS), F32)


def call(kernel, outs, scratch=()):
    return pl.pallas_call(
        kernel,
        out_shape=outs,
        scratch_shapes=list(scratch),
        name=kernel.__name__,
    )


def borders(cols, up, down):
    def shift(x, axis, by):
        count = lax.axis_size(axis)
        return lax.ppermute(x, axis, [(i, (i + by) % count) for i in range(count)])

    left = shift(cols, GX, 1)
    right = shift(cols, GX, -1)
    below = shift(up, GY, 1)
    above = shift(down, GY, -1)
    return left, right, below, above


def local(state):
    top, raw, cols, up, down = call(start_kernel, (TOPS, RAW, RAW, ROW, ROW))(state)
    halos = borders(cols, up, down)
    tops = lax.all_to_all(top, ALL, 0, 0, tiled=True)
    work = (pltpu.VMEM((7, 5, 5, 8, COLS), F32),)
    volume = call(volume_kernel, (FIELD, FIELD), work)
    high, less = volume(state)
    first, raw, cols, up, down = call(first_kernel, (FIELD, RAW, RAW, ROW, ROW))(
        tops, state, high, less, raw, *halos
    )
    halos = borders(cols, up, down)
    high, less = volume(first)
    return call(last_kernel, (FIELD, FIELD))(tops, state, first, high, less, raw, *halos)


def solution(mesh):
    torus = Mesh(mesh.devices.reshape(4, 4, 4, 2), ALL)
    return jax.shard_map(
        local,
        mesh=torus,
        in_specs=(P(None, None, None, GY, GX),),
        out_specs=(P(None, None, None, GY, GX), P(None, None, None, GY, GX)),
        check_vma=False,
    )
```

```python
import math

import jax
import jax.numpy as jnp
import numpy as np
from jax import lax
from jax.experimental import pallas as pl
from jax.experimental.pallas import tpu as pltpu
from jax.sharding import Mesh
from jax.sharding import PartitionSpec as P

GX = ("gx_0", "gx_1")
GY = ("gy_0", "gy_1")
ALL = ("gx_0", "gx_1", "gy_0", "gy_1")


ADIABATIC = 1.4
COURANT = 0.2
ALPHA_MAX = 0.5
ROWS = 16
COLS = 128
F32 = jnp.float32


def tables():
    lobatto = np.array([-1.0, -math.sqrt(3.0 / 7.0), 0.0, math.sqrt(3.0 / 7.0), 1.0])
    weights = np.array([0.1, 49.0 / 90.0, 32.0 / 45.0, 49.0 / 90.0, 0.1])
    identity = np.eye(5)
    distance = lobatto[:, None] - lobatto[None, :] + identity
    barycentric = 1.0 / np.prod(distance, axis=1)
    derivative = (1.0 - identity) * (barycentric[None, :] / barycentric[:, None]) / distance
    derivative = derivative - identity * derivative.sum(axis=1)[:, None]
    legendre = np.zeros((5, 5))
    legendre[:, 0] = 1.0
    legendre[:, 1] = lobatto
    for degree in range(2, 5):
        legendre[:, degree] = (
            (2 * degree - 1) * lobatto * legendre[:, degree - 1]
            - (degree - 1) * legendre[:, degree - 2]
        ) / degree
    norms = np.array([2.0, 2.0 / 3.0, 2.0 / 5.0, 2.0 / 7.0, 0.5])
    inverse = (legendre * weights[:, None]).T / norms[:, None]
    return derivative, weights, inverse


DERIVATIVE, WEIGHTS, INVERSE = tables()
SKEW = WEIGHTS[:, None] * DERIVATIVE
PER_WEIGHT = 1.0 / WEIGHTS
SCALE = (1.0, 0.5, 0.5, 0.5)
LN2 = math.log(2.0)


def node_values(rho, mx, my, en):
    inv_rho = 1.0 / rho
    vx = mx * inv_rho
    vy = my * inv_rho
    pressure = 0.4 * (en - 0.5 * (mx * vx + my * vy))
    return vx, vy, pressure, inv_rho


def thermal(rho, pressure, inv_rho):
    beta = rho * (1.0 / pressure)
    theta = pressure * inv_rho
    return beta, theta


class Node:
    def __init__(self, rho, vn, vt, p, beta, inv_rho, theta):
        self.rho, self.vn, self.vt, self.p = rho, vn, vt, p
        self.beta, self.inv_rho, self.theta = beta, inv_rho, theta


def pair(left, right, q):
    s = left.rho + right.rho
    d = right.rho - left.rho
    near = jnp.abs(d) < 0.01 * s
    logged = 0.5 * jnp.log(right.rho * left.inv_rho)
    t = d * (1.0 / jnp.where(near, s, logged))
    f = t * t
    series = 1.0 + f * (1.0 / 3.0 + f * (0.2 + f * (1.0 / 7.0)))
    mean2 = jnp.where(near, s * (1.0 / series), t)
    sb = left.beta + right.beta
    db = right.beta - left.beta
    nearb = jnp.abs(db) < 0.01 * sb
    loggedb = 5.0 * jnp.log(right.beta * left.theta)
    r = 1.0 / jnp.where(nearb, sb, db)
    tb = db * r
    fb = tb * tb
    seriesb = 10.0 + fb * (10.0 / 3.0 + fb * (2.0 + fb * (10.0 / 7.0)))
    warm = jnp.where(nearb, seriesb, loggedb) * r
    vn = left.vn + right.vn
    vt = left.vt + right.vt
    ps = left.p + right.p
    mass = (mean2 * vn) * (0.5 * q)
    along = mass * vn + ps * (2.0 * q)
    across = mass * vt
    dot = left.vn * right.vn + left.vt * right.vt
    energy = mass * (dot + warm) + (left.p * right.vn + right.p * left.vn) * (2.0 * q)
    return mass, along, across, energy


def line_terms(nodes, cons, speeds):
    high = [[None] * 5 for _ in range(4)]
    for i in range(5):
        for j in range(i + 1, 5):
            flux = pair(nodes[i], nodes[j], float(SKEW[i, j]))
            for v in range(4):
                high[v][i] = flux[v] if high[v][i] is None else high[v][i] + flux[v]
                high[v][j] = -flux[v] if high[v][j] is None else high[v][j] - flux[v]
    own = []
    for node, (rho, mn, mt, en) in zip(nodes, cons):
        own.append((mn, mn * node.vn + node.p, mn * node.vt, node.vn * (en + node.p)))
    less = [[None] * 5 for _ in range(4)]
    for v in range(4):
        before = None
        for i in range(4):
            spread = jnp.maximum(speeds[i], speeds[i + 1])
            inner = own[i][v] + own[i + 1][v] - spread * (cons[i + 1][v] - cons[i][v])
            if v == 0:
                inner = 0.5 * inner
            here = inner if before is None else inner - before
            less[v][i] = here - high[v][i]
            before = inner
        less[v][4] = -before - high[v][4]
    return high, less


def sound(theta):
    return jnp.sqrt(ADIABATIC * theta)


def face(left_cons, right_cons, normal):
    sides = []
    speeds = []
    for rho, mx, my, en in (left_cons, right_cons):
        vx, vy, p, inv_rho = node_values(rho, mx, my, en)
        beta, theta = thermal(rho, p, inv_rho)
        vn, vt = (vx, vy) if normal == 0 else (vy, vx)
        sides.append(Node(rho, vn, vt, p, beta, inv_rho, theta))
        speeds.append(jnp.abs(vn) + sound(theta))
    mass, along, across, energy = pair(sides[0], sides[1], 0.5)
    flux = (mass, along, across, energy) if normal == 0 else (mass, across, along, energy)
    fastest = jnp.maximum(speeds[0], speeds[1])
    out = []
    for v in range(4):
        jump = fastest * (right_cons[v] - left_cons[v])
        out.append(flux[v] - (0.5 * jump if v == 0 else jump))
    return out


def transform(values):
    s0, s1 = values[0] + values[4], values[1] + values[3]
    d0, d1 = values[0] - values[4], values[1] - values[3]
    out = []
    for k in range(5):
        c = [float(x) for x in INVERSE[k]]
        if k % 2 == 0:
            out.append(c[0] * s0 + c[1] * s1 + c[2] * values[2])
        else:
            out.append(c[0] * d0 + c[1] * d1)
    return out


def raw_indicator(indicator):
    along = [transform(indicator[a]) for a in range(5)]
    modal = [transform([along[a][l] for a in range(5)]) for l in range(5)]
    levels = [None] * 5
    for l in range(5):
        for k in range(5):
            square = modal[l][k] * modal[l][k]
            level = max(k, l)
            levels[level] = square if levels[level] is None else levels[level] + square
    lower = levels[0] + levels[1] + levels[2] + levels[3]
    total = lower + levels[4]
    energy = jnp.maximum(levels[4] / total, levels[3] / lower)
    threshold = 0.5 * 10.0 ** (-1.8 * 5.0**0.25)
    sharpness = math.log((1.0 - 0.0001) / 0.0001)
    sigmoid = 1.0 / (1.0 + jnp.exp(-sharpness / threshold * (energy - threshold)))
    return jnp.minimum(sigmoid, ALPHA_MAX)


def lanes():
    return lax.broadcasted_iota(jnp.int32, (8, COLS), 1)


def sublanes():
    return lax.broadcasted_iota(jnp.int32, (8, COLS), 0)


def pack_borders(get, raws, cols_ref, up_ref, down_ref):
    lane = lanes()
    for i in range(2):
        packed = jnp.zeros((8, COLS), F32)
        for v in range(4):
            for a in range(5):
                j = v * 5 + a
                first = get(v, a, 0, pl.ds(8 * i, 8))
                last = get(v, a, 4, pl.ds(8 * i, 8))
                packed = jnp.where(lane == j, first if j == 0 else pltpu.roll(first, j, 1), packed)
                packed = jnp.where(lane == 64 + j, pltpu.roll(last, 65 + j, 1), packed)
        packed = jnp.where(lane == 20, pltpu.roll(raws[i], 20, 1), packed)
        packed = jnp.where(lane == 84, pltpu.roll(raws[i], 85, 1), packed)
        cols_ref[pl.ds(8 * i, 8), :] = packed
    for v in range(4):
        for b in range(5):
            j = v * 5 + b
            up_ref[j : j + 1, :] = get(v, 4, b, pl.ds(15, 1))
            down_ref[j : j + 1, :] = get(v, 0, b, pl.ds(0, 1))
    up_ref[20:21, :] = raws[1][7:8, :]
    down_ref[20:21, :] = raws[0][0:1, :]
    zeros = jnp.zeros((3, COLS), F32)
    up_ref[21:24, :] = zeros
    down_ref[21:24, :] = zeros


def start_kernel(u_ref, top_ref, raw_ref, cols_ref, up_ref, down_ref):
    raws = []
    top = None
    for i in range(2):
        rows = pl.ds(8 * i, 8)
        indicator = [[None] * 5 for _ in range(5)]
        for a in range(5):
            for b in range(5):
                rho, mx, my, en = (u_ref[v, a, b, rows, :] for v in range(4))
                vx, vy, p, inv_rho = node_values(rho, mx, my, en)
                indicator[a][b] = rho * p
                speed = jnp.sqrt(vx * vx + vy * vy) + sound(p * inv_rho)
                top = speed if top is None else jnp.maximum(top, speed)
        raws.append(raw_indicator(indicator))
        raw_ref[rows, :] = raws[i]
    top_ref[...] = jnp.broadcast_to(jnp.max(top).reshape(1, 1, 1), top_ref.shape)
    pack_borders(lambda v, a, b, rows: u_ref[v, a, b, rows, :], raws, cols_ref, up_ref, down_ref)


def volume_kernel(u_ref, high_ref, less_ref, work_ref):
    def chunk(i, carry):
        rows = pl.ds(pl.multiple_of(8 * i, 8), 8)
        for a in range(5):
            for b in range(5):
                rho, mx, my, en = (u_ref[v, a, b, rows, :] for v in range(4))
                vx, vy, p, inv_rho = node_values(rho, mx, my, en)
                beta, theta = thermal(rho, p, inv_rho)
                for k, x in enumerate((vx, vy, p, beta, inv_rho, theta, sound(theta))):
                    work_ref[k, a, b] = x
        for normal in range(2):
            for across in range(5):
                nodes, cons, speeds = [], [], []
                for along in range(5):
                    a, b = (across, along) if normal == 0 else (along, across)
                    rho, mx, my, en = (u_ref[v, a, b, rows, :] for v in range(4))
                    vx, vy, p, beta, inv_rho, theta, c = (work_ref[k, a, b] for k in range(7))
                    vn, vt, mn, mt = (vx, vy, mx, my) if normal == 0 else (vy, vx, my, mx)
                    nodes.append(Node(rho, vn, vt, p, beta, inv_rho, theta))
                    cons.append((rho, mn, mt, en))
                    speeds.append(jnp.abs(vn) + c)
                high, less = line_terms(nodes, cons, speeds)
                for along in range(5):
                    a, b = (across, along) if normal == 0 else (along, across)
                    for k in range(4):
                        v = k if normal == 0 else (0, 2, 1, 3)[k]
                        scale = -float(PER_WEIGHT[along]) * SCALE[v]
                        if normal == 0:
                            high_ref[v, a, b, rows, :] = scale * high[k][along]
                            less_ref[v, a, b, rows, :] = scale * less[k][along]
                        else:
                            high_ref[v, a, b, rows, :] += scale * high[k][along]
                            less_ref[v, a, b, rows, :] += scale * less[k][along]
        return carry

    lax.fori_loop(0, 2, chunk, 0)


def rates(i, get, high_ref, less_ref, raw_ref, halo_refs, emit):
    left_ref, right_ref, below_ref, above_ref = halo_refs
    rows = pl.ds(8 * i, 8)
    lane, sublane = lanes(), sublanes()
    from_left = left_ref[rows, :]
    from_right = right_ref[rows, :]

    def from_before_x(x, j):
        return jnp.where(lane == 0, pltpu.roll(from_left, (128 - 64 - j) % 128, 1), pltpu.roll(x, 1, 1))

    def from_after_x(x, j):
        return jnp.where(lane == 127, pltpu.roll(from_right, 127 - j, 1), pltpu.roll(x, 127, 1))

    def from_before_y(x, other):
        return jnp.where(sublane == 0, jnp.broadcast_to(other, (8, COLS)), pltpu.roll(x, 1, 0))

    def from_after_y(x, other):
        return jnp.where(sublane == 7, jnp.broadcast_to(other, (8, COLS)), pltpu.roll(x, 7, 0))

    capped = raw_ref[rows, :]
    below = from_before_y(capped, below_ref[20:21, :] if i == 0 else raw_ref[7:8, :])
    above = from_after_y(capped, above_ref[20:21, :] if i == 1 else raw_ref[8:9, :])
    beside = jnp.maximum(
        jnp.maximum(below, above),
        jnp.maximum(from_before_x(capped, 20), from_after_x(capped, 20)),
    )
    blend = jnp.maximum(capped, 0.5 * beside)

    ends = {}
    for a in range(5):
        lower = [get(v, a, 0, rows) for v in range(4)]
        upper = [get(v, a, 4, rows) for v in range(4)]
        before = [from_before_x(upper[v], v * 5 + a) for v in range(4)]
        after = [from_after_x(lower[v], v * 5 + a) for v in range(4)]
        for b, flux, sign in (
            (0, face(before, lower, 0), 1.0),
            (4, face(upper, after, 0), -1.0),
        ):
            for v in range(4):
                ends[v, a, b] = (sign * float(PER_WEIGHT[b]) * SCALE[v]) * flux[v]
    for b in range(5):
        lower = [get(v, 0, b, rows) for v in range(4)]
        upper = [get(v, 4, b, rows) for v in range(4)]
        before, after = [], []
        for v in range(4):
            j = v * 5 + b
            other = below_ref[j : j + 1, :] if i == 0 else get(v, 4, b, pl.ds(7, 1))
            before.append(from_before_y(upper[v], other))
            other = above_ref[j : j + 1, :] if i == 1 else get(v, 0, b, pl.ds(8, 1))
            after.append(from_after_y(lower[v], other))
        for a, flux, sign in (
            (0, face(before, lower, 1), 1.0),
            (4, face(upper, after, 1), -1.0),
        ):
            for v in range(4):
                term = (sign * float(PER_WEIGHT[a]) * SCALE[v]) * flux[v]
                ends[v, a, b] = ends[v, a, b] + term if (v, a, b) in ends else term
    for a in range(5):
        for b in range(5):
            for v in range(4):
                rate = high_ref[v, a, b, rows, :] + blend * less_ref[v, a, b, rows, :]
                if (v, a, b) in ends:
                    rate = rate + ends[v, a, b]
                emit(v, a, b, rows, rate)


def step_of(tops_ref):
    top = tops_ref[0]
    for k in range(1, 128):
        top = jnp.maximum(top, tops_ref[k])
    return (COURANT * 2.0 / 9.0) / jnp.broadcast_to(top, (8, COLS))


def first_kernel(
    tops_ref, u_ref, high_ref, less_ref, raw_ref, left_ref, right_ref, below_ref, above_ref,
    first_ref, next_raw_ref, cols_ref, up_ref, down_ref,
):
    step = step_of(tops_ref)
    halos = (left_ref, right_ref, below_ref, above_ref)

    def get(v, a, b, rows):
        return u_ref[v, a, b, rows, :]

    def emit(v, a, b, rows, rate):
        first_ref[v, a, b, rows, :] = u_ref[v, a, b, rows, :] + step * rate

    raws = []
    for i in range(2):
        rates(i, get, high_ref, less_ref, raw_ref, halos, emit)
        rows = pl.ds(8 * i, 8)
        indicator = [[None] * 5 for _ in range(5)]
        for a in range(5):
            for b in range(5):
                rho, mx, my, en = (first_ref[v, a, b, rows, :] for v in range(4))
                indicator[a][b] = rho * node_values(rho, mx, my, en)[2]
        raws.append(raw_indicator(indicator))
        next_raw_ref[rows, :] = raws[i]
    pack_borders(
        lambda v, a, b, rows: first_ref[v, a, b, rows, :], raws, cols_ref, up_ref, down_ref
    )


def last_kernel(
    tops_ref, u_ref, first_ref, high_ref, less_ref, raw_ref, left_ref, right_ref, below_ref, above_ref,
    advanced_ref, tendency_ref,
):
    step = step_of(tops_ref)
    halos = (left_ref, right_ref, below_ref, above_ref)

    def get(v, a, b, rows):
        return first_ref[v, a, b, rows, :]

    def emit(v, a, b, rows, rate):
        tendency_ref[v, a, b, rows, :] = rate
        first = first_ref[v, a, b, rows, :] + step * rate
        advanced_ref[v, a, b, rows, :] = 0.5 * (u_ref[v, a, b, rows, :] + first)

    for i in range(2):
        rates(i, get, high_ref, less_ref, raw_ref, halos, emit)


FIELD = jax.ShapeDtypeStruct((4, 5, 5, ROWS, COLS), F32)
RAW = jax.ShapeDtypeStruct((ROWS, COLS), F32)
ROW = jax.ShapeDtypeStruct((24, COLS), F32)
TOPS = jax.ShapeDtypeStruct((128, 1, COLS), F32)


def near(x):
    return pltpu.with_memory_space_constraint(x, pltpu.VMEM)


def call(kernel, outs, scratch=(), keep=True):
    def run(*args):
        return pl.pallas_call(
            kernel,
            out_shape=tuple(pltpu.VMEM(o.shape, o.dtype) if keep else o for o in outs),
            in_specs=[pl.BlockSpec(memory_space=pltpu.VMEM) for _ in args],
            out_specs=tuple(pl.BlockSpec(memory_space=pltpu.VMEM) for _ in outs),
            scratch_shapes=list(scratch),
            compiler_params=pltpu.CompilerParams(vmem_limit_bytes=16 << 20),
            name=kernel.__name__,
        )(*(near(x) for x in args))

    return run


def borders(cols, up, down):
    def shift(x, axis, by):
        count = lax.axis_size(axis)
        return lax.ppermute(x, axis, [(i, (i + by) % count) for i in range(count)])

    left = shift(cols, GX, 1)
    right = shift(cols, GX, -1)
    below = shift(up, GY, 1)
    above = shift(down, GY, -1)
    return left, right, below, above


def local(state):
    top, raw, cols, up, down = call(start_kernel, (TOPS, RAW, RAW, ROW, ROW))(state)
    halos = borders(cols, up, down)
    tops = lax.all_to_all(top, ALL, 0, 0, tiled=True)
    work = (pltpu.VMEM((7, 5, 5, 8, COLS), F32),)
    volume = call(volume_kernel, (FIELD, FIELD), work)
    high, less = volume(state)
    first, raw, cols, up, down = call(first_kernel, (FIELD, RAW, RAW, ROW, ROW))(
        tops, state, high, less, raw, *halos
    )
    halos = borders(cols, up, down)
    high, less = volume(first)
    return call(last_kernel, (FIELD, FIELD), keep=False)(tops, state, first, high, less, raw, *halos)


def solution(mesh):
    torus = Mesh(mesh.devices.reshape(4, 4, 4, 2), ALL)
    return jax.shard_map(
        local,
        mesh=torus,
        in_specs=(P(None, None, None, GY, GX),),
        out_specs=(P(None, None, None, GY, GX), P(None, None, None, GY, GX)),
        check_vma=False,
    )
```

```python
import math

import jax
import jax.numpy as jnp
import numpy as np
from jax import lax
from jax.experimental import pallas as pl
from jax.experimental.pallas import tpu as pltpu
from jax.sharding import Mesh
from jax.sharding import PartitionSpec as P

GX = ("gx_0", "gx_1")
GY = ("gy_0", "gy_1")
ALL = ("gx_0", "gx_1", "gy_0", "gy_1")


ADIABATIC = 1.4
COURANT = 0.2
ALPHA_MAX = 0.5
ROWS = 16
COLS = 128
F32 = jnp.float32


def tables():
    lobatto = np.array([-1.0, -math.sqrt(3.0 / 7.0), 0.0, math.sqrt(3.0 / 7.0), 1.0])
    weights = np.array([0.1, 49.0 / 90.0, 32.0 / 45.0, 49.0 / 90.0, 0.1])
    identity = np.eye(5)
    distance = lobatto[:, None] - lobatto[None, :] + identity
    barycentric = 1.0 / np.prod(distance, axis=1)
    derivative = (1.0 - identity) * (barycentric[None, :] / barycentric[:, None]) / distance
    derivative = derivative - identity * derivative.sum(axis=1)[:, None]
    legendre = np.zeros((5, 5))
    legendre[:, 0] = 1.0
    legendre[:, 1] = lobatto
    for degree in range(2, 5):
        legendre[:, degree] = (
            (2 * degree - 1) * lobatto * legendre[:, degree - 1]
            - (degree - 1) * legendre[:, degree - 2]
        ) / degree
    norms = np.array([2.0, 2.0 / 3.0, 2.0 / 5.0, 2.0 / 7.0, 0.5])
    inverse = (legendre * weights[:, None]).T / norms[:, None]
    return derivative, weights, inverse


DERIVATIVE, WEIGHTS, INVERSE = tables()
SKEW = WEIGHTS[:, None] * DERIVATIVE
PER_WEIGHT = 1.0 / WEIGHTS
SCALE = (1.0, 0.5, 0.5, 0.5)
LN2 = math.log(2.0)


def node_values(rho, mx, my, en):
    inv_rho = 1.0 / rho
    vx = mx * inv_rho
    vy = my * inv_rho
    pressure = 0.4 * (en - 0.5 * (mx * vx + my * vy))
    return vx, vy, pressure, inv_rho


def thermal(rho, pressure, inv_rho):
    beta = rho * (1.0 / pressure)
    theta = pressure * inv_rho
    return beta, theta


class Node:
    def __init__(self, rho, vn, vt, p, beta, inv_rho, theta):
        self.rho, self.vn, self.vt, self.p = rho, vn, vt, p
        self.beta, self.inv_rho, self.theta = beta, inv_rho, theta


def pair(left, right, q):
    s = left.rho + right.rho
    d = right.rho - left.rho
    near = jnp.abs(d) < 0.01 * s
    logged = 0.5 * jnp.log(right.rho * left.inv_rho)
    t = d * (1.0 / jnp.where(near, s, logged))
    f = t * t
    series = 1.0 + f * (1.0 / 3.0 + f * (0.2 + f * (1.0 / 7.0)))
    mean2 = jnp.where(near, s * (1.0 / series), t)
    sb = left.beta + right.beta
    db = right.beta - left.beta
    nearb = jnp.abs(db) < 0.01 * sb
    loggedb = 5.0 * jnp.log(right.beta * left.theta)
    r = 1.0 / jnp.where(nearb, sb, db)
    tb = db * r
    fb = tb * tb
    seriesb = 10.0 + fb * (10.0 / 3.0 + fb * (2.0 + fb * (10.0 / 7.0)))
    warm = jnp.where(nearb, seriesb, loggedb) * r
    vn = left.vn + right.vn
    vt = left.vt + right.vt
    ps = left.p + right.p
    mass = (mean2 * vn) * (0.5 * q)
    along = mass * vn + ps * (2.0 * q)
    across = mass * vt
    dot = left.vn * right.vn + left.vt * right.vt
    energy = mass * (dot + warm) + (left.p * right.vn + right.p * left.vn) * (2.0 * q)
    return mass, along, across, energy


def line_terms(nodes, cons, speeds):
    high = [[None] * 5 for _ in range(4)]
    for i in range(5):
        for j in range(i + 1, 5):
            flux = pair(nodes[i], nodes[j], float(SKEW[i, j]))
            for v in range(4):
                high[v][i] = flux[v] if high[v][i] is None else high[v][i] + flux[v]
                high[v][j] = -flux[v] if high[v][j] is None else high[v][j] - flux[v]
    own = []
    for node, (rho, mn, mt, en) in zip(nodes, cons):
        own.append((mn, mn * node.vn + node.p, mn * node.vt, node.vn * (en + node.p)))
    less = [[None] * 5 for _ in range(4)]
    for v in range(4):
        before = None
        for i in range(4):
            spread = jnp.maximum(speeds[i], speeds[i + 1])
            inner = own[i][v] + own[i + 1][v] - spread * (cons[i + 1][v] - cons[i][v])
            if v == 0:
                inner = 0.5 * inner
            here = inner if before is None else inner - before
            less[v][i] = here - high[v][i]
            before = inner
        less[v][4] = -before - high[v][4]
    return high, less


def sound(theta):
    return jnp.sqrt(ADIABATIC * theta)


def face(left_cons, right_cons, normal):
    sides = []
    speeds = []
    for rho, mx, my, en in (left_cons, right_cons):
        vx, vy, p, inv_rho = node_values(rho, mx, my, en)
        beta, theta = thermal(rho, p, inv_rho)
        vn, vt = (vx, vy) if normal == 0 else (vy, vx)
        sides.append(Node(rho, vn, vt, p, beta, inv_rho, theta))
        speeds.append(jnp.abs(vn) + sound(theta))
    mass, along, across, energy = pair(sides[0], sides[1], 0.5)
    flux = (mass, along, across, energy) if normal == 0 else (mass, across, along, energy)
    fastest = jnp.maximum(speeds[0], speeds[1])
    out = []
    for v in range(4):
        jump = fastest * (right_cons[v] - left_cons[v])
        out.append(flux[v] - (0.5 * jump if v == 0 else jump))
    return out


def transform(values):
    s0, s1 = values[0] + values[4], values[1] + values[3]
    d0, d1 = values[0] - values[4], values[1] - values[3]
    out = []
    for k in range(5):
        c = [float(x) for x in INVERSE[k]]
        if k % 2 == 0:
            out.append(c[0] * s0 + c[1] * s1 + c[2] * values[2])
        else:
            out.append(c[0] * d0 + c[1] * d1)
    return out


def raw_indicator(indicator):
    along = [transform(indicator[a]) for a in range(5)]
    modal = [transform([along[a][l] for a in range(5)]) for l in range(5)]
    levels = [None] * 5
    for l in range(5):
        for k in range(5):
            square = modal[l][k] * modal[l][k]
            level = max(k, l)
            levels[level] = square if levels[level] is None else levels[level] + square
    lower = levels[0] + levels[1] + levels[2] + levels[3]
    total = lower + levels[4]
    energy = jnp.maximum(levels[4] / total, levels[3] / lower)
    threshold = 0.5 * 10.0 ** (-1.8 * 5.0**0.25)
    sharpness = math.log((1.0 - 0.0001) / 0.0001)
    sigmoid = 1.0 / (1.0 + jnp.exp(-sharpness / threshold * (energy - threshold)))
    return jnp.minimum(sigmoid, ALPHA_MAX)


def lanes():
    return lax.broadcasted_iota(jnp.int32, (8, COLS), 1)


def sublanes():
    return lax.broadcasted_iota(jnp.int32, (8, COLS), 0)


def odd_column():
    return lax.rem(lax.axis_index("gx_1"), 2)


def odd_row():
    return lax.axis_index("gy_1")


def pack_borders(get, raws, cols_ref, even_ref, odd_ref, both_ref):
    up_ref, down_ref = both_ref.at[0], both_ref.at[1]
    lane = lanes()
    for i in range(2):
        packed = jnp.zeros((8, COLS), F32)
        for v in range(4):
            for a in range(5):
                j = v * 5 + a
                first = get(v, a, 0, pl.ds(8 * i, 8))
                last = get(v, a, 4, pl.ds(8 * i, 8))
                packed = jnp.where(lane == j, first if j == 0 else pltpu.roll(first, j, 1), packed)
                packed = jnp.where(lane == 64 + j, pltpu.roll(last, 65 + j, 1), packed)
        packed = jnp.where(lane == 20, pltpu.roll(raws[i], 20, 1), packed)
        packed = jnp.where(lane == 84, pltpu.roll(raws[i], 85, 1), packed)
        cols_ref[pl.ds(8 * i, 8), :] = packed
    for v in range(4):
        for b in range(5):
            j = v * 5 + b
            up_ref[j : j + 1, :] = get(v, 4, b, pl.ds(15, 1))
            down_ref[j : j + 1, :] = get(v, 0, b, pl.ds(0, 1))
    up_ref[20:21, :] = raws[1][7:8, :]
    down_ref[20:21, :] = raws[0][0:1, :]
    zeros = jnp.zeros((3, COLS), F32)
    up_ref[21:24, :] = zeros
    down_ref[21:24, :] = zeros
    odd = odd_row()
    even_ref[...] = both_ref[odd]
    odd_ref[...] = both_ref[1 - odd]


def unpack_borders(col_even_ref, col_odd_ref, row_even_ref, row_odd_ref, cols_ref, rows_ref):
    cols_ref[0] = col_even_ref[...]
    cols_ref[1] = col_odd_ref[...]
    rows_ref[0] = row_even_ref[...]
    rows_ref[1] = row_odd_ref[...]
    odd = odd_column()
    left, right = cols_ref.at[1 - odd], cols_ref.at[odd]
    odd = odd_row()
    below, above = rows_ref.at[1 - odd], rows_ref.at[odd]
    return left, right, below, above


def start_kernel(u_ref, top_ref, raw_ref, cols_ref, even_ref, odd_ref, both_ref):
    raws = []
    top = None
    for i in range(2):
        rows = pl.ds(8 * i, 8)
        indicator = [[None] * 5 for _ in range(5)]
        for a in range(5):
            for b in range(5):
                rho, mx, my, en = (u_ref[v, a, b, rows, :] for v in range(4))
                vx, vy, p, inv_rho = node_values(rho, mx, my, en)
                indicator[a][b] = rho * p
                speed = jnp.sqrt(vx * vx + vy * vy) + sound(p * inv_rho)
                top = speed if top is None else jnp.maximum(top, speed)
        raws.append(raw_indicator(indicator))
        raw_ref[rows, :] = raws[i]
    top_ref[...] = jnp.broadcast_to(jnp.max(top).reshape(1, 1, 1), top_ref.shape)
    pack_borders(lambda v, a, b, rows: u_ref[v, a, b, rows, :], raws, cols_ref, even_ref, odd_ref, both_ref)


def volume_kernel(u_ref, high_ref, less_ref, work_ref):
    def chunk(i, carry):
        rows = pl.ds(pl.multiple_of(8 * i, 8), 8)
        for a in range(5):
            for b in range(5):
                rho, mx, my, en = (u_ref[v, a, b, rows, :] for v in range(4))
                vx, vy, p, inv_rho = node_values(rho, mx, my, en)
                beta, theta = thermal(rho, p, inv_rho)
                for k, x in enumerate((vx, vy, p, beta, inv_rho, theta, sound(theta))):
                    work_ref[k, a, b] = x
        for normal in range(2):
            for across in range(5):
                nodes, cons, speeds = [], [], []
                for along in range(5):
                    a, b = (across, along) if normal == 0 else (along, across)
                    rho, mx, my, en = (u_ref[v, a, b, rows, :] for v in range(4))
                    vx, vy, p, beta, inv_rho, theta, c = (work_ref[k, a, b] for k in range(7))
                    vn, vt, mn, mt = (vx, vy, mx, my) if normal == 0 else (vy, vx, my, mx)
                    nodes.append(Node(rho, vn, vt, p, beta, inv_rho, theta))
                    cons.append((rho, mn, mt, en))
                    speeds.append(jnp.abs(vn) + c)
                high, less = line_terms(nodes, cons, speeds)
                for along in range(5):
                    a, b = (across, along) if normal == 0 else (along, across)
                    for k in range(4):
                        v = k if normal == 0 else (0, 2, 1, 3)[k]
                        scale = -float(PER_WEIGHT[along]) * SCALE[v]
                        if normal == 0:
                            high_ref[v, a, b, rows, :] = scale * high[k][along]
                            less_ref[v, a, b, rows, :] = scale * less[k][along]
                        else:
                            high_ref[v, a, b, rows, :] += scale * high[k][along]
                            less_ref[v, a, b, rows, :] += scale * less[k][along]
        return carry

    lax.fori_loop(0, 2, chunk, 0)


def rates(i, get, high_ref, less_ref, raw_ref, halo_refs, emit):
    left_ref, right_ref, below_ref, above_ref = halo_refs
    rows = pl.ds(8 * i, 8)
    lane, sublane = lanes(), sublanes()
    from_left = left_ref[rows, :]
    from_right = right_ref[rows, :]

    def from_before_x(x, j):
        return jnp.where(lane == 0, pltpu.roll(from_left, (128 - 64 - j) % 128, 1), pltpu.roll(x, 1, 1))

    def from_after_x(x, j):
        return jnp.where(lane == 127, pltpu.roll(from_right, 127 - j, 1), pltpu.roll(x, 127, 1))

    def from_before_y(x, other):
        return jnp.where(sublane == 0, jnp.broadcast_to(other, (8, COLS)), pltpu.roll(x, 1, 0))

    def from_after_y(x, other):
        return jnp.where(sublane == 7, jnp.broadcast_to(other, (8, COLS)), pltpu.roll(x, 7, 0))

    capped = raw_ref[rows, :]
    below = from_before_y(capped, below_ref[20:21, :] if i == 0 else raw_ref[7:8, :])
    above = from_after_y(capped, above_ref[20:21, :] if i == 1 else raw_ref[8:9, :])
    beside = jnp.maximum(
        jnp.maximum(below, above),
        jnp.maximum(from_before_x(capped, 20), from_after_x(capped, 20)),
    )
    blend = jnp.maximum(capped, 0.5 * beside)

    ends = {}
    for a in range(5):
        lower = [get(v, a, 0, rows) for v in range(4)]
        upper = [get(v, a, 4, rows) for v in range(4)]
        before = [from_before_x(upper[v], v * 5 + a) for v in range(4)]
        after = [from_after_x(lower[v], v * 5 + a) for v in range(4)]
        for b, flux, sign in (
            (0, face(before, lower, 0), 1.0),
            (4, face(upper, after, 0), -1.0),
        ):
            for v in range(4):
                ends[v, a, b] = (sign * float(PER_WEIGHT[b]) * SCALE[v]) * flux[v]
    for b in range(5):
        lower = [get(v, 0, b, rows) for v in range(4)]
        upper = [get(v, 4, b, rows) for v in range(4)]
        before, after = [], []
        for v in range(4):
            j = v * 5 + b
            other = below_ref[j : j + 1, :] if i == 0 else get(v, 4, b, pl.ds(7, 1))
            before.append(from_before_y(upper[v], other))
            other = above_ref[j : j + 1, :] if i == 1 else get(v, 0, b, pl.ds(8, 1))
            after.append(from_after_y(lower[v], other))
        for a, flux, sign in (
            (0, face(before, lower, 1), 1.0),
            (4, face(upper, after, 1), -1.0),
        ):
            for v in range(4):
                term = (sign * float(PER_WEIGHT[a]) * SCALE[v]) * flux[v]
                ends[v, a, b] = ends[v, a, b] + term if (v, a, b) in ends else term
    for a in range(5):
        for b in range(5):
            for v in range(4):
                rate = high_ref[v, a, b, rows, :] + blend * less_ref[v, a, b, rows, :]
                if (v, a, b) in ends:
                    rate = rate + ends[v, a, b]
                emit(v, a, b, rows, rate)


def step_of(tops_ref):
    top = tops_ref[0]
    for k in range(1, 128):
        top = jnp.maximum(top, tops_ref[k])
    return (COURANT * 2.0 / 9.0) / jnp.broadcast_to(top, (8, COLS))


def first_kernel(
    tops_ref, u_ref, high_ref, less_ref, raw_ref, col_even_ref, col_odd_ref, row_even_ref, row_odd_ref,
    first_ref, next_raw_ref, cols_ref, even_ref, odd_ref, both_ref, got_cols_ref, got_rows_ref,
):
    step = step_of(tops_ref)
    halos = unpack_borders(
        col_even_ref, col_odd_ref, row_even_ref, row_odd_ref, got_cols_ref, got_rows_ref
    )

    def get(v, a, b, rows):
        return u_ref[v, a, b, rows, :]

    def emit(v, a, b, rows, rate):
        first_ref[v, a, b, rows, :] = u_ref[v, a, b, rows, :] + step * rate

    raws = []
    for i in range(2):
        rates(i, get, high_ref, less_ref, raw_ref, halos, emit)
        rows = pl.ds(8 * i, 8)
        indicator = [[None] * 5 for _ in range(5)]
        for a in range(5):
            for b in range(5):
                rho, mx, my, en = (first_ref[v, a, b, rows, :] for v in range(4))
                indicator[a][b] = rho * node_values(rho, mx, my, en)[2]
        raws.append(raw_indicator(indicator))
        next_raw_ref[rows, :] = raws[i]
    pack_borders(
        lambda v, a, b, rows: first_ref[v, a, b, rows, :],
        raws, cols_ref, even_ref, odd_ref, both_ref,
    )


def last_kernel(
    tops_ref, u_ref, first_ref, high_ref, less_ref, raw_ref, col_even_ref, col_odd_ref, row_even_ref, row_odd_ref,
    advanced_ref, tendency_ref, got_cols_ref, got_rows_ref,
):
    step = step_of(tops_ref)
    halos = unpack_borders(
        col_even_ref, col_odd_ref, row_even_ref, row_odd_ref, got_cols_ref, got_rows_ref
    )

    def get(v, a, b, rows):
        return first_ref[v, a, b, rows, :]

    def emit(v, a, b, rows, rate):
        tendency_ref[v, a, b, rows, :] = rate
        first = first_ref[v, a, b, rows, :] + step * rate
        advanced_ref[v, a, b, rows, :] = 0.5 * (u_ref[v, a, b, rows, :] + first)

    for i in range(2):
        rates(i, get, high_ref, less_ref, raw_ref, halos, emit)


FIELD = jax.ShapeDtypeStruct((4, 5, 5, ROWS, COLS), F32)
RAW = jax.ShapeDtypeStruct((ROWS, COLS), F32)
ROW = jax.ShapeDtypeStruct((24, COLS), F32)
TOPS = jax.ShapeDtypeStruct((128, 1, COLS), F32)


def near(x):
    return pltpu.with_memory_space_constraint(x, pltpu.VMEM)


def call(kernel, outs, scratch=(), keep=True):
    def run(*args):
        return pl.pallas_call(
            kernel,
            out_shape=tuple(pltpu.VMEM(o.shape, o.dtype) if keep else o for o in outs),
            in_specs=[pl.BlockSpec(memory_space=pltpu.VMEM) for _ in args],
            out_specs=tuple(pl.BlockSpec(memory_space=pltpu.VMEM) for _ in outs),
            scratch_shapes=list(scratch),
            compiler_params=pltpu.CompilerParams(vmem_limit_bytes=16 << 20),
            name=kernel.__name__,
        )(*(near(x) for x in args))

    return run


BOTH = pltpu.VMEM((2, 24, COLS), F32)
GOT = (pltpu.VMEM((2, ROWS, COLS), F32), pltpu.VMEM((2, 24, COLS), F32))


def borders(cols, even, odd):
    def swap(x, axis, second):
        count = lax.axis_size(axis)
        pairs = [(i, (((i + second) ^ 1) - second) % count) for i in range(count)]
        return lax.ppermute(x, axis, pairs)

    return swap(cols, GX, 0), swap(cols, GX, 1), swap(even, GY, 0), swap(odd, GY, 1)


def local(state):
    top, raw, cols, even, odd = call(start_kernel, (TOPS, RAW, RAW, ROW, ROW), (BOTH,))(state)
    halos = borders(cols, even, odd)
    tops = lax.all_to_all(top, ALL, 0, 0, tiled=True)
    volume = call(volume_kernel, (FIELD, FIELD), (pltpu.VMEM((7, 5, 5, 8, COLS), F32),))
    high, less = volume(state)
    first, raw, cols, even, odd = call(
        first_kernel, (FIELD, RAW, RAW, ROW, ROW), (BOTH, *GOT)
    )(tops, state, high, less, raw, *halos)
    halos = borders(cols, even, odd)
    high, less = volume(first)
    return call(last_kernel, (FIELD, FIELD), GOT, keep=False)(
        tops, state, first, high, less, raw, *halos
    )


def solution(mesh):
    torus = Mesh(mesh.devices.reshape(4, 4, 4, 2), ALL)
    return jax.shard_map(
        local,
        mesh=torus,
        in_specs=(P(None, None, None, GY, GX),),
        out_specs=(P(None, None, None, GY, GX), P(None, None, None, GY, GX)),
        check_vma=False,
    )
```

```python
import math

import jax
import jax.numpy as jnp
import numpy as np
from jax import lax
from jax.experimental import pallas as pl
from jax.experimental.pallas import tpu as pltpu
from jax.sharding import Mesh
from jax.sharding import PartitionSpec as P

GX = ("gx_0", "gx_1")
GY = ("gy_0", "gy_1")
ALL = ("gx_0", "gx_1", "gy_0", "gy_1")


ADIABATIC = 1.4
COURANT = 0.2
ALPHA_MAX = 0.5
ROWS = 16
COLS = 128
F32 = jnp.float32


def tables():
    lobatto = np.array([-1.0, -math.sqrt(3.0 / 7.0), 0.0, math.sqrt(3.0 / 7.0), 1.0])
    weights = np.array([0.1, 49.0 / 90.0, 32.0 / 45.0, 49.0 / 90.0, 0.1])
    identity = np.eye(5)
    distance = lobatto[:, None] - lobatto[None, :] + identity
    barycentric = 1.0 / np.prod(distance, axis=1)
    derivative = (1.0 - identity) * (barycentric[None, :] / barycentric[:, None]) / distance
    derivative = derivative - identity * derivative.sum(axis=1)[:, None]
    legendre = np.zeros((5, 5))
    legendre[:, 0] = 1.0
    legendre[:, 1] = lobatto
    for degree in range(2, 5):
        legendre[:, degree] = (
            (2 * degree - 1) * lobatto * legendre[:, degree - 1]
            - (degree - 1) * legendre[:, degree - 2]
        ) / degree
    norms = np.array([2.0, 2.0 / 3.0, 2.0 / 5.0, 2.0 / 7.0, 0.5])
    inverse = (legendre * weights[:, None]).T / norms[:, None]
    return derivative, weights, inverse


DERIVATIVE, WEIGHTS, INVERSE = tables()
SKEW = WEIGHTS[:, None] * DERIVATIVE
PER_WEIGHT = 1.0 / WEIGHTS
SCALE = (1.0, 0.5, 0.5, 0.5)
LN2 = math.log(2.0)


LN2 = math.log(2.0)
NEAR = math.log2(1.01 / 0.99)


def velocity_pressure(rho, mx, my, en):
    inv_rho = 1.0 / rho
    vx = mx * inv_rho
    vy = my * inv_rho
    pressure = 0.4 * en - 0.2 * (mx * vx + my * vy)
    return vx, vy, pressure, inv_rho


def sound(theta):
    square = (ADIABATIC / (5.0 * LN2)) * theta
    return square * lax.rsqrt(square)


def derived(rho, mx, my, en):
    vx, vy, p, inv_rho = velocity_pressure(rho, mx, my, en)
    theta = (5.0 * LN2) * (p * inv_rho)
    return vx, vy, p, rho * ((0.2 / LN2) / p), theta, inv_rho, sound(theta)


class Node:
    def __init__(self, cons, values, normal):
        rho, mx, my, en = cons
        vx, vy, p, beta, theta, inv_rho, c = values
        self.rho, self.en, self.p = rho, en, p
        self.beta, self.theta, self.inv_rho = beta, theta, inv_rho
        self.vn, self.vt, self.mn, self.mt = (vx, vy, mx, my) if normal == 0 else (vy, vx, my, mx)
        self.speed = jnp.abs(self.vn) + c
        self.cons = (rho, self.mn, self.mt, en)


def series(f):
    c = [2.0 / (k * LN2) for k in (1, 3, 5, 7)]
    return c[0] + f * (c[1] + f * (c[2] + f * c[3]))


def pair(left, right, q):
    s = left.rho + right.rho
    d = right.rho - left.rho
    logged = lax.log2(right.rho * left.inv_rho)
    near = jnp.abs(logged) < NEAR
    t = d * (1.0 / jnp.where(near, s, logged))
    mean = jnp.where(near, s * (1.0 / series(t * t)), t)
    s = left.beta + right.beta
    d = right.beta - left.beta
    logged = lax.log2(right.beta * left.theta)
    near = jnp.abs(logged) < NEAR
    r = 1.0 / jnp.where(near, s, d)
    t = d * r
    warm = jnp.where(near, series(t * t), logged) * r
    vn = left.vn + right.vn
    vt = left.vt + right.vt
    ps = left.p + right.p
    cross = left.p * right.vn + right.p * left.vn
    if q != 0.5:
        ps = ps * (2.0 * q)
        cross = cross * (2.0 * q)
    mass = (mean * vn) * (q / LN2)
    along = mass * vn + ps
    across = mass * vt
    dot = left.vn * right.vn + left.vt * right.vt
    energy = mass * (dot + warm) + cross
    return mass, along, across, energy


def line_terms(nodes):
    high = [[None] * 5 for _ in range(4)]
    for j in range(4, 0, -1):
        for i in range(j):
            flux = pair(nodes[i], nodes[j], float(SKEW[i, j]))
            for v in range(4):
                high[v][i] = flux[v] if high[v][i] is None else high[v][i] + flux[v]
                if j == 4:
                    high[v][4] = flux[v] if high[v][4] is None else high[v][4] + flux[v]
                else:
                    high[v][j] = high[v][j] - flux[v]
    own = []
    for node in nodes:
        flow = node.mn * node.vn + node.p
        own.append((node.mn, flow, node.mn * node.vt, node.vn * (node.en + node.p)))
    low = [[None] * 5 for _ in range(4)]
    for v in range(4):
        before = None
        for i in range(4):
            spread = jnp.maximum(nodes[i].speed, nodes[i + 1].speed)
            jump = nodes[i + 1].cons[v] - nodes[i].cons[v]
            inner = own[i][v] + own[i + 1][v] - spread * jump
            low[v][i] = inner if before is None else inner - before
            before = inner
        low[v][4] = before
    return high, low


def face(left, right):
    flux = pair(left, right, 0.5)
    fastest = jnp.maximum(left.speed, right.speed)
    out = []
    for v in range(4):
        jump = fastest * (right.cons[v] - left.cons[v])
        out.append(flux[v] - (0.5 * jump if v == 0 else jump))
    return out


def transform(values):
    s0, s1 = values[0] + values[4], values[1] + values[3]
    d0, d1 = values[0] - values[4], values[1] - values[3]
    out = []
    for k in range(5):
        c = [float(x) for x in INVERSE[k]]
        if k % 2 == 0:
            out.append(c[0] * s0 + c[1] * s1 + c[2] * values[2])
        else:
            out.append(c[0] * d0 + c[1] * d1)
    return out


def raw_indicator(indicator):
    along = [transform(indicator[a]) for a in range(5)]
    modal = [transform([along[a][l] for a in range(5)]) for l in range(5)]
    levels = [None] * 5
    for l in range(5):
        for k in range(5):
            square = modal[l][k] * modal[l][k]
            level = max(k, l)
            levels[level] = square if levels[level] is None else levels[level] + square
    lower = levels[0] + levels[1] + levels[2] + levels[3]
    total = lower + levels[4]
    energy = jnp.maximum(levels[4] / total, levels[3] / lower)
    threshold = 0.5 * 10.0 ** (-1.8 * 5.0**0.25)
    sharpness = math.log((1.0 - 0.0001) / 0.0001)
    sigmoid = 1.0 / (1.0 + jnp.exp(-sharpness / threshold * (energy - threshold)))
    return jnp.minimum(sigmoid, ALPHA_MAX)


def lanes():
    return lax.broadcasted_iota(jnp.int32, (8, COLS), 1)


def sublanes():
    return lax.broadcasted_iota(jnp.int32, (8, COLS), 0)


def odd_column():
    return lax.rem(lax.axis_index("gx_1"), 2)


def odd_row():
    return lax.axis_index("gy_1")


def pack_borders(get, raws, cols_ref, even_ref, odd_ref, both_ref):
    up_ref, down_ref = both_ref.at[0], both_ref.at[1]
    lane = lanes()
    for i in range(2):
        packed = jnp.zeros((8, COLS), F32)
        for v in range(4):
            for a in range(5):
                j = v * 5 + a
                first = get(v, a, 0, pl.ds(8 * i, 8))
                last = get(v, a, 4, pl.ds(8 * i, 8))
                packed = jnp.where(lane == j, first if j == 0 else pltpu.roll(first, j, 1), packed)
                packed = jnp.where(lane == 64 + j, pltpu.roll(last, 65 + j, 1), packed)
        packed = jnp.where(lane == 20, pltpu.roll(raws[i], 20, 1), packed)
        packed = jnp.where(lane == 84, pltpu.roll(raws[i], 85, 1), packed)
        cols_ref[pl.ds(8 * i, 8), :] = packed
    for v in range(4):
        for b in range(5):
            j = v * 5 + b
            up_ref[j : j + 1, :] = get(v, 4, b, pl.ds(15, 1))
            down_ref[j : j + 1, :] = get(v, 0, b, pl.ds(0, 1))
    up_ref[20:21, :] = raws[1][7:8, :]
    down_ref[20:21, :] = raws[0][0:1, :]
    zeros = jnp.zeros((3, COLS), F32)
    up_ref[21:24, :] = zeros
    down_ref[21:24, :] = zeros
    odd = odd_row()
    even_ref[...] = both_ref[odd]
    odd_ref[...] = both_ref[1 - odd]


def unpack_borders(col_even_ref, col_odd_ref, row_even_ref, row_odd_ref, cols_ref, rows_ref):
    cols_ref[0] = col_even_ref[...]
    cols_ref[1] = col_odd_ref[...]
    rows_ref[0] = row_even_ref[...]
    rows_ref[1] = row_odd_ref[...]
    odd = odd_column()
    left, right = cols_ref.at[1 - odd], cols_ref.at[odd]
    odd = odd_row()
    below, above = rows_ref.at[1 - odd], rows_ref.at[odd]
    return left, right, below, above


def start_kernel(u_ref, top_ref, raw_ref, cols_ref, even_ref, odd_ref, both_ref):
    raws = []
    top = None
    for i in range(2):
        rows = pl.ds(8 * i, 8)
        indicator = [[None] * 5 for _ in range(5)]
        for a in range(5):
            for b in range(5):
                cons = [u_ref[v, a, b, rows, :] for v in range(4)]
                vx, vy, p, _, _, _, c = derived(*cons)
                indicator[a][b] = cons[0] * p
                speed = jnp.sqrt(vx * vx + vy * vy) + c
                top = speed if top is None else jnp.maximum(top, speed)
        raws.append(raw_indicator(indicator))
        raw_ref[rows, :] = raws[i]
    top_ref[...] = jnp.broadcast_to(jnp.max(top).reshape(1, 1, 1), top_ref.shape)
    pack_borders(
        lambda v, a, b, rows: u_ref[v, a, b, rows, :], raws, cols_ref, even_ref, odd_ref, both_ref
    )


ORDER = ((0, 1, 2, 3), (0, 2, 1, 3))


def volume_kernel(u_ref, work_ref, high_ref, low_ref):
    def chunk(i, carry):
        rows = pl.ds(pl.multiple_of(8 * i, 8), 8)
        for normal in range(2):
            for across in range(5):
                places = [(across, k) if normal == 0 else (k, across) for k in range(5)]
                nodes = []
                for a, b in places:
                    cons = [u_ref[v, a, b, rows, :] for v in range(4)]
                    nodes.append(Node(cons, [work_ref[k, a, b, rows, :] for k in range(7)], normal))
                sums = line_terms(nodes)
                for ref, terms in zip((high_ref, low_ref), sums):
                    for along, (a, b) in enumerate(places):
                        for k in range(4):
                            v = ORDER[normal][k]
                            term = terms[k][along]
                            if normal == 1:
                                ratio = float(WEIGHTS[b] / WEIGHTS[a])
                                if a not in (b, 4 - b):
                                    term = ratio * term
                                before = ref[v, a, b, rows, :]
                                term = before - term if (a == 4) != (b == 4) else before + term
                            ref[v, a, b, rows, :] = term
        return carry

    lax.fori_loop(0, 2, chunk, 0)


def first_volume_kernel(u_ref, high_ref, low_ref, work_ref):
    def chunk(i, carry):
        rows = pl.ds(pl.multiple_of(8 * i, 8), 8)
        for a in range(5):
            for b in range(5):
                for k, x in enumerate(derived(*(u_ref[v, a, b, rows, :] for v in range(4)))):
                    work_ref[k, a, b, rows, :] = x
        return carry

    lax.fori_loop(0, 2, chunk, 0)
    volume_kernel(u_ref, work_ref, high_ref, low_ref)


def rates(i, get, work_ref, high_ref, low_ref, raw_ref, halos, emit):
    left_ref, right_ref, below_ref, above_ref = halos
    rows = pl.ds(8 * i, 8)
    lane, sublane = lanes(), sublanes()
    from_left = left_ref[rows, :]
    from_right = right_ref[rows, :]

    def from_before_x(x, j):
        return jnp.where(
            lane == 0, pltpu.roll(from_left, (128 - 64 - j) % 128, 1), pltpu.roll(x, 1, 1)
        )

    def from_after_x(x, j):
        return jnp.where(lane == 127, pltpu.roll(from_right, 127 - j, 1), pltpu.roll(x, 127, 1))

    def from_before_y(x, other):
        return jnp.where(sublane == 0, jnp.broadcast_to(other, (8, COLS)), pltpu.roll(x, 1, 0))

    def from_after_y(x, other):
        return jnp.where(sublane == 7, jnp.broadcast_to(other, (8, COLS)), pltpu.roll(x, 7, 0))

    capped = raw_ref[rows, :]
    below = from_before_y(capped, below_ref[20:21, :] if i == 0 else raw_ref[7:8, :])
    above = from_after_y(capped, above_ref[20:21, :] if i == 1 else raw_ref[8:9, :])
    beside = jnp.maximum(
        jnp.maximum(below, above),
        jnp.maximum(from_before_x(capped, 20), from_after_x(capped, 20)),
    )
    blend = jnp.maximum(capped, 0.5 * beside)
    rest = 1.0 - blend
    shares = (0.5 * blend, blend, blend, blend)

    def own(a, b, normal):
        cons = [get(v, a, b, rows) for v in range(4)]
        if work_ref is None:
            return cons, Node(cons, derived(*cons), normal)
        return cons, Node(cons, [work_ref[k, a, b, rows, :] for k in range(7)], normal)

    def other(cons, normal):
        return Node(cons, derived(*cons), normal)

    ends = {}
    for a in range(5):
        cons, lower = own(a, 0, 0)
        after = other([from_after_x(cons[v], v * 5 + a) for v in range(4)], 0)
        cons, upper = own(a, 4, 0)
        before = other([from_before_x(cons[v], v * 5 + a) for v in range(4)], 0)
        for b, flux in ((0, face(before, lower)), (4, face(upper, after))):
            for v in range(4):
                ends[v, a, b] = flux[v]
    for b in range(5):
        cons, lower = own(0, b, 1)
        after = []
        for v in range(4):
            j = v * 5 + b
            row = above_ref[j : j + 1, :] if i == 1 else get(v, 0, b, pl.ds(8, 1))
            after.append(from_after_y(cons[v], row))
        cons, upper = own(4, b, 1)
        before = []
        for v in range(4):
            j = v * 5 + b
            row = below_ref[j : j + 1, :] if i == 0 else get(v, 4, b, pl.ds(7, 1))
            before.append(from_before_y(cons[v], row))
        for a, flux in (
            (0, face(other(before, 1), lower)),
            (4, face(upper, other(after, 1))),
        ):
            ratio = float(WEIGHTS[b] / WEIGHTS[a])
            for k in range(4):
                v = ORDER[1][k]
                term = flux[k] if b in (0, 4) else ratio * flux[k]
                if (v, a, b) in ends:
                    same = (a == 4) == (b == 4)
                    ends[v, a, b] = ends[v, a, b] + term if same else ends[v, a, b] - term
                else:
                    ends[v, a, b] = term if a == 0 else -term
    for a in range(5):
        for b in range(5):
            for v in range(4):
                x = rest * high_ref[v, a, b, rows, :] + shares[v] * low_ref[v, a, b, rows, :]
                if (v, a, b) in ends:
                    x = x - ends[v, a, b]
                emit(v, a, b, rows, x)


def final(v, b):
    return (1.0 if b == 4 else -1.0) * float(PER_WEIGHT[b]) * SCALE[v]


def step_of(tops_ref):
    top = tops_ref[0]
    for k in range(1, 128):
        top = jnp.maximum(top, tops_ref[k])
    return (COURANT * 2.0 / 9.0) / jnp.broadcast_to(top, (8, COLS))


def first_kernel(
    tops_ref, u_ref, high_ref, low_ref, raw_ref, col_even_ref, col_odd_ref, row_even_ref, row_odd_ref,
    first_ref, next_raw_ref, next_work_ref, cols_ref, even_ref, odd_ref, both_ref, got_cols_ref, got_rows_ref,
):
    step = step_of(tops_ref)
    steps = {(v, b): final(v, b) * step for v in (0, 1) for b in range(5)}
    halos = unpack_borders(
        col_even_ref, col_odd_ref, row_even_ref, row_odd_ref, got_cols_ref, got_rows_ref
    )

    def get(v, a, b, rows):
        return u_ref[v, a, b, rows, :]

    def emit(v, a, b, rows, x):
        first_ref[v, a, b, rows, :] = u_ref[v, a, b, rows, :] + steps[min(v, 1), b] * x

    raws = []
    for i in range(2):
        rates(i, get, None, high_ref, low_ref, raw_ref, halos, emit)
        rows = pl.ds(8 * i, 8)
        indicator = [[None] * 5 for _ in range(5)]
        for a in range(5):
            for b in range(5):
                cons = [first_ref[v, a, b, rows, :] for v in range(4)]
                values = derived(*cons)
                for k, x in enumerate(values):
                    next_work_ref[k, a, b, rows, :] = x
                indicator[a][b] = cons[0] * values[2]
        raws.append(raw_indicator(indicator))
        next_raw_ref[rows, :] = raws[i]
    pack_borders(
        lambda v, a, b, rows: first_ref[v, a, b, rows, :],
        raws, cols_ref, even_ref, odd_ref, both_ref,
    )


def last_kernel(
    tops_ref, u_ref, first_ref, work_ref, high_ref, low_ref, raw_ref, col_even_ref, col_odd_ref, row_even_ref, row_odd_ref,
    advanced_ref, tendency_ref, got_cols_ref, got_rows_ref,
):
    step = step_of(tops_ref)
    halos = unpack_borders(
        col_even_ref, col_odd_ref, row_even_ref, row_odd_ref, got_cols_ref, got_rows_ref
    )

    def get(v, a, b, rows):
        return first_ref[v, a, b, rows, :]

    def emit(v, a, b, rows, x):
        rate = final(v, b) * x
        tendency_ref[v, a, b, rows, :] = rate
        first = first_ref[v, a, b, rows, :] + step * rate
        advanced_ref[v, a, b, rows, :] = 0.5 * (u_ref[v, a, b, rows, :] + first)

    for i in range(2):
        rates(i, get, work_ref, high_ref, low_ref, raw_ref, halos, emit)


FIELD = jax.ShapeDtypeStruct((4, 5, 5, ROWS, COLS), F32)
RAW = jax.ShapeDtypeStruct((ROWS, COLS), F32)
ROW = jax.ShapeDtypeStruct((24, COLS), F32)
WORK = jax.ShapeDtypeStruct((7, 5, 5, ROWS, COLS), F32)
TOPS = jax.ShapeDtypeStruct((128, 1, COLS), F32)


def near(x):
    return pltpu.with_memory_space_constraint(x, pltpu.VMEM)


def call(kernel, outs, scratch=(), keep=True):
    def run(*args):
        return pl.pallas_call(
            kernel,
            out_shape=tuple(pltpu.VMEM(o.shape, o.dtype) if keep else o for o in outs),
            in_specs=[pl.BlockSpec(memory_space=pltpu.VMEM) for _ in args],
            out_specs=tuple(pl.BlockSpec(memory_space=pltpu.VMEM) for _ in outs),
            scratch_shapes=list(scratch),
            compiler_params=pltpu.CompilerParams(vmem_limit_bytes=16 << 20),
            name=kernel.__name__,
        )(*(near(x) for x in args))

    return run


BOTH = pltpu.VMEM((2, 24, COLS), F32)
GOT = (pltpu.VMEM((2, ROWS, COLS), F32), pltpu.VMEM((2, 24, COLS), F32))


def borders(cols, even, odd):
    def swap(x, axis, second):
        count = lax.axis_size(axis)
        pairs = [(i, (((i + second) ^ 1) - second) % count) for i in range(count)]
        return lax.ppermute(x, axis, pairs)

    return swap(cols, GX, 0), swap(cols, GX, 1), swap(even, GY, 0), swap(odd, GY, 1)


def local(state):
    top, raw, cols, even, odd = call(start_kernel, (TOPS, RAW, RAW, ROW, ROW), (BOTH,))(state)
    halos = borders(cols, even, odd)
    tops = lax.all_to_all(top, ALL, 0, 0, tiled=True)
    work = pltpu.VMEM(WORK.shape, F32)
    high, low = call(first_volume_kernel, (FIELD, FIELD), (work,))(state)
    first, raw, work, cols, even, odd = call(
        first_kernel, (FIELD, RAW, WORK, RAW, ROW, ROW), (BOTH, *GOT)
    )(tops, state, high, low, raw, *halos)
    halos = borders(cols, even, odd)
    high, low = call(volume_kernel, (FIELD, FIELD))(first, work)
    return call(last_kernel, (FIELD, FIELD), GOT, keep=False)(
        tops, state, first, work, high, low, raw, *halos
    )


def solution(mesh):
    torus = Mesh(mesh.devices.reshape(4, 4, 4, 2), ALL)
    return jax.shard_map(
        local,
        mesh=torus,
        in_specs=(P(None, None, None, GY, GX),),
        out_specs=(P(None, None, None, GY, GX), P(None, None, None, GY, GX)),
        check_vma=False,
    )
```

```python
import math

import jax
import jax.numpy as jnp
import numpy as np
from jax import lax
from jax.experimental import pallas as pl
from jax.experimental.pallas import tpu as pltpu
from jax.sharding import Mesh
from jax.sharding import PartitionSpec as P

GX = ("gx_0", "gx_1")
GY = ("gy_0", "gy_1")
ALL = ("gx_0", "gx_1", "gy_0", "gy_1")


ADIABATIC = 1.4
COURANT = 0.2
ALPHA_MAX = 0.5
ROWS = 16
COLS = 128
F32 = jnp.float32


def tables():
    lobatto = np.array([-1.0, -math.sqrt(3.0 / 7.0), 0.0, math.sqrt(3.0 / 7.0), 1.0])
    weights = np.array([0.1, 49.0 / 90.0, 32.0 / 45.0, 49.0 / 90.0, 0.1])
    identity = np.eye(5)
    distance = lobatto[:, None] - lobatto[None, :] + identity
    barycentric = 1.0 / np.prod(distance, axis=1)
    derivative = (1.0 - identity) * (barycentric[None, :] / barycentric[:, None]) / distance
    derivative = derivative - identity * derivative.sum(axis=1)[:, None]
    legendre = np.zeros((5, 5))
    legendre[:, 0] = 1.0
    legendre[:, 1] = lobatto
    for degree in range(2, 5):
        legendre[:, degree] = (
            (2 * degree - 1) * lobatto * legendre[:, degree - 1]
            - (degree - 1) * legendre[:, degree - 2]
        ) / degree
    norms = np.array([2.0, 2.0 / 3.0, 2.0 / 5.0, 2.0 / 7.0, 0.5])
    inverse = (legendre * weights[:, None]).T / norms[:, None]
    return derivative, weights, inverse


DERIVATIVE, WEIGHTS, INVERSE = tables()
SKEW = WEIGHTS[:, None] * DERIVATIVE
PER_WEIGHT = 1.0 / WEIGHTS
SCALE = (1.0, 0.5, 0.5, 0.5)
LN2 = math.log(2.0)


LN2 = math.log(2.0)
NEAR = math.log2(1.01 / 0.99)


def velocity_pressure(rho, mx, my, en):
    inv_rho = 1.0 / rho
    vx = mx * inv_rho
    vy = my * inv_rho
    pressure = 0.4 * en - 0.2 * (mx * vx + my * vy)
    return vx, vy, pressure, inv_rho


def sound(theta):
    square = (ADIABATIC / (5.0 * LN2)) * theta
    return square * lax.rsqrt(square)


def derived(rho, mx, my, en):
    vx, vy, p, inv_rho = velocity_pressure(rho, mx, my, en)
    theta = (5.0 * LN2) * (p * inv_rho)
    return vx, vy, p, rho * ((0.2 / LN2) / p), theta, inv_rho, sound(theta)


class Node:
    def __init__(self, cons, values, normal):
        rho, mx, my, en = cons
        vx, vy, p, beta, theta, inv_rho, c = values
        self.rho, self.en, self.p = rho, en, p
        self.beta, self.theta, self.inv_rho = beta, theta, inv_rho
        self.vn, self.vt, self.mn, self.mt = (vx, vy, mx, my) if normal == 0 else (vy, vx, my, mx)
        self.speed = jnp.abs(self.vn) + c
        self.cons = (rho, self.mn, self.mt, en)


def series(f):
    c = [2.0 / (k * LN2) for k in (1, 3, 5, 7)]
    return c[0] + f * (c[1] + f * (c[2] + f * c[3]))


def pair(left, right, q):
    s = left.rho + right.rho
    d = right.rho - left.rho
    logged = lax.log2(right.rho * left.inv_rho)
    near = jnp.abs(logged) < NEAR
    t = d * (1.0 / jnp.where(near, s, logged))
    mean = jnp.where(near, s * (1.0 / series(t * t)), t)
    s = left.beta + right.beta
    d = right.beta - left.beta
    logged = lax.log2(right.beta * left.theta)
    near = jnp.abs(logged) < NEAR
    r = 1.0 / jnp.where(near, s, d)
    t = d * r
    warm = jnp.where(near, series(t * t), logged) * r
    vn = left.vn + right.vn
    vt = left.vt + right.vt
    ps = left.p + right.p
    cross = left.p * right.vn + right.p * left.vn
    if q != 0.5:
        ps = ps * (2.0 * q)
        cross = cross * (2.0 * q)
    mass = (mean * vn) * (q / LN2)
    along = mass * vn + ps
    across = mass * vt
    dot = left.vn * right.vn + left.vt * right.vt
    energy = mass * (dot + warm) + cross
    return mass, along, across, energy


def line_terms(nodes, lower, upper):
    high = [[None] * 5 for _ in range(4)]
    for j in range(4, 0, -1):
        for i in range(j):
            flux = pair(nodes[i], nodes[j], float(SKEW[i, j]))
            for v in range(4):
                high[v][i] = flux[v] if high[v][i] is None else high[v][i] + flux[v]
                if j == 4:
                    high[v][4] = flux[v] if high[v][4] is None else high[v][4] + flux[v]
                else:
                    high[v][j] = high[v][j] - flux[v]
    own = []
    for node in nodes:
        flow = node.mn * node.vn + node.p
        own.append((node.mn, flow, node.mn * node.vt, node.vn * (node.en + node.p)))
    low = [[None] * 5 for _ in range(4)]
    for v in range(4):
        before = None
        for i in range(4):
            spread = jnp.maximum(nodes[i].speed, nodes[i + 1].speed)
            jump = nodes[i + 1].cons[v] - nodes[i].cons[v]
            inner = own[i][v] + own[i + 1][v] - spread * jump
            low[v][i] = inner if before is None else inner - before
            before = inner
        low[v][4] = before
        for i, flux in ((0, lower[v]), (4, upper[v])):
            high[v][i] = high[v][i] - flux
            low[v][i] = low[v][i] - (flux + flux if v == 0 else flux)
    return high, low


def face(left, right):
    flux = pair(left, right, 0.5)
    fastest = jnp.maximum(left.speed, right.speed)
    out = []
    for v in range(4):
        jump = fastest * (right.cons[v] - left.cons[v])
        out.append(flux[v] - (0.5 * jump if v == 0 else jump))
    return out


def transform(values):
    s0, s1 = values[0] + values[4], values[1] + values[3]
    d0, d1 = values[0] - values[4], values[1] - values[3]
    out = []
    for k in range(5):
        c = [float(x) for x in INVERSE[k]]
        if k % 2 == 0:
            out.append(c[0] * s0 + c[1] * s1 + c[2] * values[2])
        else:
            out.append(c[0] * d0 + c[1] * d1)
    return out


def raw_indicator(indicator):
    along = [transform(indicator[a]) for a in range(5)]
    modal = [transform([along[a][l] for a in range(5)]) for l in range(5)]
    levels = [None] * 5
    for l in range(5):
        for k in range(5):
            square = modal[l][k] * modal[l][k]
            level = max(k, l)
            levels[level] = square if levels[level] is None else levels[level] + square
    lower = levels[0] + levels[1] + levels[2] + levels[3]
    total = lower + levels[4]
    energy = jnp.maximum(levels[4] / total, levels[3] / lower)
    threshold = 0.5 * 10.0 ** (-1.8 * 5.0**0.25)
    sharpness = math.log((1.0 - 0.0001) / 0.0001)
    sigmoid = 1.0 / (1.0 + jnp.exp(-sharpness / threshold * (energy - threshold)))
    return jnp.minimum(sigmoid, ALPHA_MAX)


def lanes():
    return lax.broadcasted_iota(jnp.int32, (8, COLS), 1)


def sublanes():
    return lax.broadcasted_iota(jnp.int32, (8, COLS), 0)


def odd_column():
    return lax.rem(lax.axis_index("gx_1"), 2)


def odd_row():
    return lax.axis_index("gy_1")


def pack_borders(get, raws, cols_ref, even_ref, odd_ref, both_ref):
    up_ref, down_ref = both_ref.at[0], both_ref.at[1]
    lane = lanes()
    for i in range(2):
        packed = jnp.zeros((8, COLS), F32)
        for v in range(4):
            for a in range(5):
                j = v * 5 + a
                first = get(v, a, 0, pl.ds(8 * i, 8))
                last = get(v, a, 4, pl.ds(8 * i, 8))
                packed = jnp.where(lane == j, first if j == 0 else pltpu.roll(first, j, 1), packed)
                packed = jnp.where(lane == 64 + j, pltpu.roll(last, 65 + j, 1), packed)
        packed = jnp.where(lane == 20, pltpu.roll(raws[i], 20, 1), packed)
        packed = jnp.where(lane == 84, pltpu.roll(raws[i], 85, 1), packed)
        cols_ref[pl.ds(8 * i, 8), :] = packed
    for v in range(4):
        for b in range(5):
            j = v * 5 + b
            up_ref[j : j + 1, :] = get(v, 4, b, pl.ds(15, 1))
            down_ref[j : j + 1, :] = get(v, 0, b, pl.ds(0, 1))
    up_ref[20:21, :] = raws[1][7:8, :]
    down_ref[20:21, :] = raws[0][0:1, :]
    zeros = jnp.zeros((3, COLS), F32)
    up_ref[21:24, :] = zeros
    down_ref[21:24, :] = zeros
    odd = odd_row()
    even_ref[...] = both_ref[odd]
    odd_ref[...] = both_ref[1 - odd]


def unpack_borders(col_even_ref, col_odd_ref, row_even_ref, row_odd_ref, cols_ref, rows_ref):
    cols_ref[0] = col_even_ref[...]
    cols_ref[1] = col_odd_ref[...]
    rows_ref[0] = row_even_ref[...]
    rows_ref[1] = row_odd_ref[...]
    odd = odd_column()
    left, right = cols_ref.at[1 - odd], cols_ref.at[odd]
    odd = odd_row()
    below, above = rows_ref.at[1 - odd], rows_ref.at[odd]
    return left, right, below, above


def own_borders(cols_ref, even_ref, odd_ref, rows_ref):
    rows_ref[0] = even_ref[...]
    rows_ref[1] = odd_ref[...]
    odd = odd_row()
    return cols_ref, (rows_ref.at[1 - odd], rows_ref.at[odd])


def start_kernel(state_ref, top_ref, u_ref, arrived):
    copies = [
        pltpu.make_async_copy(state_ref.at[:, a], u_ref.at[:, a], arrived.at[a]) for a in range(5)
    ]
    for copy in copies:
        copy.start()
    tops = [None, None]
    for a in range(5):
        copies[a].wait()
        for i in range(2):
            rows = pl.ds(8 * i, 8)
            for b in range(5):
                rho, mx, my, en = (u_ref[v, a, b, rows, :] for v in range(4))
                vx, vy, p, inv_rho = velocity_pressure(rho, mx, my, en)
                square = vx * vx + vy * vy
                speed = square * lax.rsqrt(jnp.maximum(square, 1e-37))
                square = ADIABATIC * (p * inv_rho)
                speed = speed + square * lax.rsqrt(square)
                tops[i] = speed if tops[i] is None else jnp.maximum(tops[i], speed)
    top = jnp.max(jnp.maximum(tops[0], tops[1]))
    top_ref[...] = jnp.broadcast_to(top.reshape(1, 1, 1), top_ref.shape)


def border_kernel(u_ref, raw_ref, cols_ref, even_ref, odd_ref, both_ref):
    raws = []
    for i in range(2):
        rows = pl.ds(8 * i, 8)
        indicator = [[None] * 5 for _ in range(5)]
        for a in range(5):
            for b in range(5):
                cons = [u_ref[v, a, b, rows, :] for v in range(4)]
                indicator[a][b] = cons[0] * velocity_pressure(*cons)[2]
        raws.append(raw_indicator(indicator))
        raw_ref[rows, :] = raws[i]
    pack_borders(
        lambda v, a, b, rows: u_ref[v, a, b, rows, :], raws, cols_ref, even_ref, odd_ref, both_ref
    )


ORDER = ((0, 1, 2, 3), (0, 2, 1, 3))


def node_at(u_ref, work_ref, a, b, normal, load):
    cons = [load(u_ref, (v, a, b)) for v in range(4)]
    return Node(cons, [load(work_ref, (k, a, b)) for k in range(7)], normal)


def row_faces(u_ref, work_ref, faces_ref):
    sublane = sublanes()
    for b in range(5):
        fluxes = []
        for i in range(2):
            rows = pl.ds(8 * i, 8)

            def above(ref, index, i=i):
                if i == 0:
                    return ref[(*index, pl.ds(1, 8), slice(None))]
                return pltpu.roll(ref[(*index, pl.ds(8, 8), slice(None))], 7, 0)

            def here(ref, index, rows=rows):
                return ref[(*index, rows, slice(None))]

            left = node_at(u_ref, work_ref, 4, b, 1, here)
            right = node_at(u_ref, work_ref, 0, b, 1, above)
            fluxes.append(face(left, right))
        for v in range(4):
            first = fluxes[0][v]
            second = jnp.where(sublane == 7, 0.0, fluxes[1][v])
            rolled = pltpu.roll(first, 1, 0)
            faces_ref[0, v, b, 0:8, :] = jnp.where(sublane == 0, 0.0, rolled)
            faces_ref[0, v, b, 8:16, :] = jnp.where(sublane == 0, rolled, pltpu.roll(second, 1, 0))
            faces_ref[1, v, b, 0:8, :] = first
            faces_ref[1, v, b, 8:16, :] = second


def volume_kernel(u_ref, work_ref, high_ref, low_ref, faces_ref):
    row_faces(u_ref, work_ref, faces_ref)
    lane = lanes()

    def chunk(i, carry):
        rows = pl.ds(pl.multiple_of(8 * i, 8), 8)

        def here(ref, index):
            return ref[(*index, rows, slice(None))]

        def after(ref, index):
            return pltpu.roll(here(ref, index), 127, 1)

        for normal in range(2):
            for across in range(5):
                places = [(across, k) if normal == 0 else (k, across) for k in range(5)]
                nodes = [node_at(u_ref, work_ref, a, b, normal, here) for a, b in places]
                if normal == 0:
                    flux = face(nodes[4], node_at(u_ref, work_ref, across, 0, 0, after))
                    upper = [jnp.where(lane == 127, 0.0, x) for x in flux]
                    lower = [pltpu.roll(x, 1, 1) for x in upper]
                else:
                    lower, upper = (
                        [faces_ref[k, v, across, rows, :] for v in range(4)] for k in range(2)
                    )
                sums = line_terms(nodes, lower, upper)
                for ref, terms in zip((high_ref, low_ref), sums):
                    for along, (a, b) in enumerate(places):
                        for k in range(4):
                            v = ORDER[normal][k]
                            term = terms[k][along]
                            if normal == 1:
                                ratio = float(WEIGHTS[b] / WEIGHTS[a])
                                if a not in (b, 4 - b):
                                    term = ratio * term
                                before = ref[v, a, b, rows, :]
                                term = before - term if (a == 4) != (b == 4) else before + term
                            ref[v, a, b, rows, :] = term
        return carry

    lax.fori_loop(0, 2, chunk, 0)


def first_volume_kernel(u_ref, high_ref, low_ref, work_ref, faces_ref):
    def chunk(i, carry):
        rows = pl.ds(pl.multiple_of(8 * i, 8), 8)
        for a in range(5):
            for b in range(5):
                for k, x in enumerate(derived(*(u_ref[v, a, b, rows, :] for v in range(4)))):
                    work_ref[k, a, b, rows, :] = x
        return carry

    lax.fori_loop(0, 2, chunk, 0)
    volume_kernel(u_ref, work_ref, high_ref, low_ref, faces_ref)


def plain(cons, normal):
    return Node(cons, derived(*cons), normal)


def rates(i, high_ref, low_ref, raw_ref, mine, halos, edge_ref, emit, finish=None):
    my_cols_ref, my_rows_ref = mine
    left_ref, right_ref, below_ref, above_ref = halos
    rows = pl.ds(8 * i, 8)
    lane, sublane = lanes(), sublanes()
    from_left, from_right, own = left_ref[rows, :], right_ref[rows, :], my_cols_ref[rows, :]

    capped = raw_ref[rows, :]
    row_before = below_ref[20:21, :] if i == 0 else raw_ref[7:8, :]
    row_after = above_ref[20:21, :] if i == 1 else raw_ref[8:9, :]
    below = jnp.where(sublane == 0, jnp.broadcast_to(row_before, (8, COLS)), pltpu.roll(capped, 1, 0))
    above = jnp.where(sublane == 7, jnp.broadcast_to(row_after, (8, COLS)), pltpu.roll(capped, 7, 0))
    before = jnp.where(lane == 0, pltpu.roll(from_left, 44, 1), pltpu.roll(capped, 1, 1))
    after = jnp.where(lane == 127, pltpu.roll(from_right, 107, 1), pltpu.roll(capped, 127, 1))
    beside = jnp.maximum(jnp.maximum(below, above), jnp.maximum(before, after))
    blend = jnp.maximum(capped, 0.5 * beside)
    rest = 1.0 - blend
    shares = (0.5 * blend, blend, blend, blend)

    lefts, rights = [], []
    for v in range(4):
        shifted = own if v == 0 else pltpu.roll(own, COLS - 5 * v, 1)
        lefts.append(jnp.where(lane < 64, pltpu.roll(from_left, 64 - 5 * v, 1), shifted))
        rights.append(jnp.where(lane < 64, shifted, pltpu.roll(from_right, 64 - 5 * v, 1)))
    used = jnp.bitwise_and(lane, 63) < 5
    filler = (1.0, 0.0, 0.0, 1.0)
    lefts = [jnp.where(used, x, y) for x, y in zip(lefts, filler)]
    rights = [jnp.where(used, x, y) for x, y in zip(rights, filler)]
    ends = {}
    flux = face(plain(lefts, 0), plain(rights, 0))
    for v in range(4):
        for a in range(5):
            turned = flux[v] if a == 0 else pltpu.roll(flux[v], COLS - a, 1)
            ends[v, a, 0] = jnp.where(lane == 0, turned, 0.0)
            ends[v, a, 4] = jnp.where(lane == 127, pltpu.roll(flux[v], 63 - a, 1), 0.0)
    a = 4 * i
    other_ref = (below_ref, above_ref)[i]
    mine_at = my_rows_ref[i]
    other = [other_ref[5 * v : 5 * v + 5, :] for v in range(4)]
    here = [mine_at[5 * v : 5 * v + 5, :] for v in range(4)]
    sides = (plain(other, 1), plain(here, 1)) if i == 0 else (plain(here, 1), plain(other, 1))
    flux = face(*sides)
    edge = sublane == 7 * i
    for k in range(4):
        v = ORDER[1][k]
        edge_ref[8 * v : 8 * v + 5, :] = flux[k]
        for b in range(5):
            term = jnp.broadcast_to(edge_ref[8 * v + b : 8 * v + b + 1, :], (8, COLS))
            if b not in (0, 4):
                term = float(WEIGHTS[b] / WEIGHTS[a]) * term
            term = jnp.where(edge, term, 0.0)
            same = (a == 4) == (b == 4)
            if (v, a, b) in ends:
                ends[v, a, b] = ends[v, a, b] + term if same else ends[v, a, b] - term
            else:
                ends[v, a, b] = term if a == 0 else -term
    for a in range(5):
        for b in range(5):
            for v in range(4):
                x = rest * high_ref[v, a, b, rows, :] + shares[v] * low_ref[v, a, b, rows, :]
                if (v, a, b) in ends:
                    x = x - ends[v, a, b]
                emit(v, a, b, rows, x)
        if finish is not None:
            finish(a, rows)


def final(v, b):
    return (1.0 if b == 4 else -1.0) * float(PER_WEIGHT[b]) * SCALE[v]


def step_of(tops_ref):
    tops = [tops_ref[k] for k in range(128)]
    while len(tops) > 1:
        tops = [jnp.maximum(x, y) for x, y in zip(tops[::2], tops[1::2])]
    return (COURANT * 2.0 / 9.0) / jnp.broadcast_to(tops[0], (8, COLS))


def first_kernel(
    tops_ref, u_ref, high_ref, low_ref, raw_ref, my_cols_ref, my_even_ref, my_odd_ref, col_even_ref, col_odd_ref, row_even_ref, row_odd_ref,
    step_ref, first_ref, next_raw_ref, next_work_ref, cols_ref, even_ref, odd_ref, both_ref, got_cols_ref, got_rows_ref, my_rows_ref, edge_ref,
):
    step = step_of(tops_ref)
    step_ref[...] = step
    steps = {(v, b): final(v, b) * step for v in (0, 1) for b in range(5)}
    halos = unpack_borders(
        col_even_ref, col_odd_ref, row_even_ref, row_odd_ref, got_cols_ref, got_rows_ref
    )

    mine = own_borders(my_cols_ref, my_even_ref, my_odd_ref, my_rows_ref)

    def emit(v, a, b, rows, x):
        first_ref[v, a, b, rows, :] = u_ref[v, a, b, rows, :] + steps[min(v, 1), b] * x

    raws = []
    for i in range(2):
        rates(i, high_ref, low_ref, raw_ref, mine, halos, edge_ref, emit)
        rows = pl.ds(8 * i, 8)
        indicator = [[None] * 5 for _ in range(5)]
        for a in range(5):
            for b in range(5):
                cons = [first_ref[v, a, b, rows, :] for v in range(4)]
                values = derived(*cons)
                for k, x in enumerate(values):
                    next_work_ref[k, a, b, rows, :] = x
                indicator[a][b] = cons[0] * values[2]
        raws.append(raw_indicator(indicator))
        next_raw_ref[rows, :] = raws[i]
    pack_borders(
        lambda v, a, b, rows: first_ref[v, a, b, rows, :],
        raws, cols_ref, even_ref, odd_ref, both_ref,
    )


def last_kernel(
    step_ref, u_ref, first_ref, high_ref, low_ref, raw_ref, my_cols_ref, my_even_ref, my_odd_ref, col_even_ref, col_odd_ref, row_even_ref, row_odd_ref,
    advanced_ref, tendency_ref, got_cols_ref, got_rows_ref, my_rows_ref, edge_ref, advanced_vmem, tendency_vmem, sent,
):
    half = 0.5 * step_ref[...]
    halos = unpack_borders(
        col_even_ref, col_odd_ref, row_even_ref, row_odd_ref, got_cols_ref, got_rows_ref
    )
    mine = own_borders(my_cols_ref, my_even_ref, my_odd_ref, my_rows_ref)
    copies = []

    def emit(v, a, b, rows, x):
        rate = final(v, b) * x
        tendency_vmem[v, a, b, rows, :] = rate
        sum_of_states = u_ref[v, a, b, rows, :] + first_ref[v, a, b, rows, :]
        advanced_vmem[v, a, b, rows, :] = 0.5 * sum_of_states + half * rate

    def finish(a, rows):
        for kept, out in ((advanced_vmem, advanced_ref), (tendency_vmem, tendency_ref)):
            copies.append(
                pltpu.make_async_copy(
                    kept.at[:, a, :, rows, :], out.at[:, a, :, rows, :], sent.at[len(copies)]
                )
            )
            copies[-1].start()

    for i in range(2):
        rates(i, high_ref, low_ref, raw_ref, mine, halos, edge_ref, emit, finish)
    for copy in copies:
        copy.wait()


FIELD = jax.ShapeDtypeStruct((4, 5, 5, ROWS, COLS), F32)
RAW = jax.ShapeDtypeStruct((ROWS, COLS), F32)
ROW = jax.ShapeDtypeStruct((24, COLS), F32)
WORK = jax.ShapeDtypeStruct((7, 5, 5, ROWS, COLS), F32)
TILE = jax.ShapeDtypeStruct((8, COLS), F32)
TOPS = jax.ShapeDtypeStruct((128, 1, COLS), F32)


def call(kernel, outs, scratch=(), hbm_in=False, hbm_out=False):
    here, there = pl.BlockSpec(memory_space=pltpu.VMEM), pl.BlockSpec(memory_space=pltpu.HBM)

    def run(*args):
        space = pltpu.HBM if hbm_in else pltpu.VMEM
        args = [pltpu.with_memory_space_constraint(x, space) for x in args]
        return pl.pallas_call(
            kernel,
            out_shape=tuple(o if hbm_out else pltpu.VMEM(o.shape, o.dtype) for o in outs),
            in_specs=[there if hbm_in else here for _ in args],
            out_specs=tuple(there if hbm_out else here for _ in outs),
            scratch_shapes=list(scratch),
            compiler_params=pltpu.CompilerParams(vmem_limit_bytes=16 << 20),
            name=kernel.__name__,
        )(*args)

    return run


BOTH = pltpu.VMEM((2, 24, COLS), F32)
GOT = (
    pltpu.VMEM((2, ROWS, COLS), F32),
    pltpu.VMEM((2, 24, COLS), F32),
    pltpu.VMEM((2, 24, COLS), F32),
    pltpu.VMEM((32, COLS), F32),
)
FACES = pltpu.VMEM((2, 4, 5, ROWS, COLS), F32)


def borders(cols, even, odd):
    def swap(x, axis, second):
        count = lax.axis_size(axis)
        pairs = [(i, (((i + second) ^ 1) - second) % count) for i in range(count)]
        return lax.ppermute(x, axis, pairs)

    return swap(cols, GX, 0), swap(cols, GX, 1), swap(even, GY, 0), swap(odd, GY, 1)


def local(state):
    top, state = call(
        start_kernel, (TOPS, FIELD), (pltpu.SemaphoreType.DMA((5,)),), hbm_in=True
    )(state)
    tops = lax.all_to_all(top, ALL, 0, 0, tiled=True)
    raw, *mine = call(border_kernel, (RAW, RAW, ROW, ROW), (BOTH,))(state)
    halos = borders(*mine)
    work = pltpu.VMEM(WORK.shape, F32)
    high, low = call(first_volume_kernel, (FIELD, FIELD), (work, FACES))(state)
    step, first, raw, work, *next_mine = call(
        first_kernel, (TILE, FIELD, RAW, WORK, RAW, ROW, ROW), (BOTH, *GOT)
    )(tops, state, high, low, raw, *mine, *halos)
    halos = borders(*next_mine)
    high, low = call(volume_kernel, (FIELD, FIELD), (FACES,))(first, work)
    kept = pltpu.VMEM(FIELD.shape, F32)
    return call(
        last_kernel, (FIELD, FIELD), (*GOT, kept, kept, pltpu.SemaphoreType.DMA((20,))), hbm_out=True
    )(step, state, first, high, low, raw, *next_mine, *halos)


def solution(mesh):
    torus = Mesh(mesh.devices.reshape(4, 4, 4, 2), ALL)
    return jax.shard_map(
        local,
        mesh=torus,
        in_specs=(P(None, None, None, GY, GX),),
        out_specs=(P(None, None, None, GY, GX), P(None, None, None, GY, GX)),
        check_vma=False,
    )
```

```python
import math

import jax
import jax.numpy as jnp
import numpy as np
from jax import lax
from jax.experimental import pallas as pl
from jax.experimental.pallas import tpu as pltpu
from jax.sharding import Mesh
from jax.sharding import PartitionSpec as P


GX = ("gx_0", "gx_1")
GY = ("gy_0", "gy_1")
ALL = ("gx_0", "gx_1", "gy_0", "gy_1")


ADIABATIC = 1.4
COURANT = 0.2
ALPHA_MAX = 0.5
ROWS = 16
COLS = 128
F32 = jnp.float32


def tables():
    lobatto = np.array([-1.0, -math.sqrt(3.0 / 7.0), 0.0, math.sqrt(3.0 / 7.0), 1.0])
    weights = np.array([0.1, 49.0 / 90.0, 32.0 / 45.0, 49.0 / 90.0, 0.1])
    identity = np.eye(5)
    distance = lobatto[:, None] - lobatto[None, :] + identity
    barycentric = 1.0 / np.prod(distance, axis=1)
    derivative = (1.0 - identity) * (barycentric[None, :] / barycentric[:, None]) / distance
    derivative = derivative - identity * derivative.sum(axis=1)[:, None]
    legendre = np.zeros((5, 5))
    legendre[:, 0] = 1.0
    legendre[:, 1] = lobatto
    for degree in range(2, 5):
        legendre[:, degree] = (
            (2 * degree - 1) * lobatto * legendre[:, degree - 1]
            - (degree - 1) * legendre[:, degree - 2]
        ) / degree
    norms = np.array([2.0, 2.0 / 3.0, 2.0 / 5.0, 2.0 / 7.0, 0.5])
    inverse = (legendre * weights[:, None]).T / norms[:, None]
    return derivative, weights, inverse


DERIVATIVE, WEIGHTS, INVERSE = tables()
SKEW = WEIGHTS[:, None] * DERIVATIVE
PER_WEIGHT = 1.0 / WEIGHTS
SCALE = (1.0, 0.5, 0.5, 0.5)
LN2 = math.log(2.0)


LN2 = math.log(2.0)
NEAR = math.log2(1.01 / 0.99)


def velocity_pressure(rho, mx, my, en):
    inv_rho = 1.0 / rho
    vx = mx * inv_rho
    vy = my * inv_rho
    pressure = 0.4 * en - 0.2 * (mx * vx + my * vy)
    return vx, vy, pressure, inv_rho


def sound(theta):
    square = (ADIABATIC / (5.0 * LN2)) * theta
    return square * lax.rsqrt(square)


def derived(rho, mx, my, en):
    vx, vy, p, inv_rho = velocity_pressure(rho, mx, my, en)
    theta = (5.0 * LN2) * (p * inv_rho)
    return vx, vy, p, rho * ((0.2 / LN2) / p), theta, inv_rho, sound(theta)


class Node:
    def __init__(self, cons, values, normal):
        rho, mx, my, en = cons
        vx, vy, p, beta, theta, inv_rho, c = values
        self.rho, self.en, self.p = rho, en, p
        self.beta, self.theta, self.inv_rho = beta, theta, inv_rho
        self.vn, self.vt, self.mn, self.mt = (vx, vy, mx, my) if normal == 0 else (vy, vx, my, mx)
        self.speed = jnp.abs(self.vn) + c
        self.cons = (rho, self.mn, self.mt, en)


def series(f):
    c = [2.0 / (k * LN2) for k in (1, 3, 5, 7)]
    return c[0] + f * (c[1] + f * (c[2] + f * c[3]))


def pair(left, right, q):
    s = left.rho + right.rho
    d = right.rho - left.rho
    logged = lax.log2(right.rho * left.inv_rho)
    near = jnp.abs(logged) < NEAR
    t = d * (1.0 / jnp.where(near, s, logged))
    mean = jnp.where(near, s * (1.0 / series(t * t)), t)
    s = left.beta + right.beta
    d = right.beta - left.beta
    logged = lax.log2(right.beta * left.theta)
    near = jnp.abs(logged) < NEAR
    r = 1.0 / jnp.where(near, s, d)
    t = d * r
    warm = jnp.where(near, series(t * t), logged) * r
    vn = left.vn + right.vn
    vt = left.vt + right.vt
    ps = left.p + right.p
    cross = left.p * right.vn + right.p * left.vn
    if q != 0.5:
        ps = ps * (2.0 * q)
        cross = cross * (2.0 * q)
    mass = (mean * vn) * (q / LN2)
    along = mass * vn + ps
    across = mass * vt
    dot = left.vn * right.vn + left.vt * right.vt
    energy = mass * (dot + warm) + cross
    return mass, along, across, energy


def line_terms(nodes, lower, upper):
    high = [[None] * 5 for _ in range(4)]
    for j in range(4, 0, -1):
        for i in range(j):
            flux = pair(nodes[i], nodes[j], float(SKEW[i, j]))
            for v in range(4):
                high[v][i] = flux[v] if high[v][i] is None else high[v][i] + flux[v]
                if j == 4:
                    high[v][4] = flux[v] if high[v][4] is None else high[v][4] + flux[v]
                else:
                    high[v][j] = high[v][j] - flux[v]
    own = []
    for node in nodes:
        flow = node.mn * node.vn + node.p
        own.append((node.mn, flow, node.mn * node.vt, node.vn * (node.en + node.p)))
    low = [[None] * 5 for _ in range(4)]
    for v in range(4):
        before = None
        for i in range(4):
            spread = jnp.maximum(nodes[i].speed, nodes[i + 1].speed)
            jump = nodes[i + 1].cons[v] - nodes[i].cons[v]
            inner = own[i][v] + own[i + 1][v] - spread * jump
            low[v][i] = inner if before is None else inner - before
            before = inner
        low[v][4] = before
        for i, flux in ((0, lower[v]), (4, upper[v])):
            high[v][i] = high[v][i] - flux
            low[v][i] = low[v][i] - (flux + flux if v == 0 else flux)
    return high, low


def face(left, right):
    flux = pair(left, right, 0.5)
    fastest = jnp.maximum(left.speed, right.speed)
    out = []
    for v in range(4):
        jump = fastest * (right.cons[v] - left.cons[v])
        out.append(flux[v] - (0.5 * jump if v == 0 else jump))
    return out


def transform(values):
    s0, s1 = values[0] + values[4], values[1] + values[3]
    d0, d1 = values[0] - values[4], values[1] - values[3]
    out = []
    for k in range(5):
        c = [float(x) for x in INVERSE[k]]
        if k % 2 == 0:
            out.append(c[0] * s0 + c[1] * s1 + c[2] * values[2])
        else:
            out.append(c[0] * d0 + c[1] * d1)
    return out


def raw_indicator(indicator):
    along = [transform(indicator[a]) for a in range(5)]
    modal = [transform([along[a][l] for a in range(5)]) for l in range(5)]
    levels = [None] * 5
    for l in range(5):
        for k in range(5):
            square = modal[l][k] * modal[l][k]
            level = max(k, l)
            levels[level] = square if levels[level] is None else levels[level] + square
    lower = levels[0] + levels[1] + levels[2] + levels[3]
    total = lower + levels[4]
    energy = jnp.maximum(levels[4] / total, levels[3] / lower)
    threshold = 0.5 * 10.0 ** (-1.8 * 5.0**0.25)
    sharpness = math.log((1.0 - 0.0001) / 0.0001)
    sigmoid = 1.0 / (1.0 + jnp.exp(-sharpness / threshold * (energy - threshold)))
    return jnp.minimum(sigmoid, ALPHA_MAX)


def lanes():
    return lax.broadcasted_iota(jnp.int32, (8, COLS), 1)


def sublanes():
    return lax.broadcasted_iota(jnp.int32, (8, COLS), 0)


def odd_column():
    return lax.rem(lax.axis_index("gx_1"), 2)


def odd_row():
    return lax.axis_index("gy_1")


def pack_borders(get, raws, cols_ref, even_ref, odd_ref, both_ref):
    up_ref, down_ref = both_ref.at[0], both_ref.at[1]
    lane = lanes()
    for i in range(2):
        packed = jnp.zeros((8, COLS), F32)
        for v in range(4):
            for a in range(5):
                j = v * 5 + a
                first = get(v, a, 0, pl.ds(8 * i, 8))
                last = get(v, a, 4, pl.ds(8 * i, 8))
                packed = jnp.where(lane == j, first if j == 0 else pltpu.roll(first, j, 1), packed)
                packed = jnp.where(lane == 64 + j, pltpu.roll(last, 65 + j, 1), packed)
        packed = jnp.where(lane == 20, pltpu.roll(raws[i], 20, 1), packed)
        packed = jnp.where(lane == 84, pltpu.roll(raws[i], 85, 1), packed)
        cols_ref[pl.ds(8 * i, 8), :] = packed
    for v in range(4):
        for b in range(5):
            j = v * 5 + b
            up_ref[j : j + 1, :] = get(v, 4, b, pl.ds(15, 1))
            down_ref[j : j + 1, :] = get(v, 0, b, pl.ds(0, 1))
    up_ref[20:21, :] = raws[1][7:8, :]
    down_ref[20:21, :] = raws[0][0:1, :]
    zeros = jnp.zeros((3, COLS), F32)
    up_ref[21:24, :] = zeros
    down_ref[21:24, :] = zeros
    odd = odd_row()
    even_ref[...] = both_ref[odd]
    odd_ref[...] = both_ref[1 - odd]


def unpack_borders(col_even_ref, col_odd_ref, row_even_ref, row_odd_ref, cols_ref, rows_ref):
    cols_ref[0] = col_even_ref[...]
    cols_ref[1] = col_odd_ref[...]
    rows_ref[0] = row_even_ref[...]
    rows_ref[1] = row_odd_ref[...]
    odd = odd_column()
    left, right = cols_ref.at[1 - odd], cols_ref.at[odd]
    odd = odd_row()
    below, above = rows_ref.at[1 - odd], rows_ref.at[odd]
    return left, right, below, above


def own_borders(cols_ref, even_ref, odd_ref, rows_ref):
    rows_ref[0] = even_ref[...]
    rows_ref[1] = odd_ref[...]
    odd = odd_row()
    return cols_ref, (rows_ref.at[1 - odd], rows_ref.at[odd])


def start_kernel(state_ref, top_ref, u_ref, arrived):
    copies = [
        pltpu.make_async_copy(state_ref.at[:, a], u_ref.at[:, a], arrived.at[a]) for a in range(5)
    ]
    for copy in copies:
        copy.start()
    tops = [None, None]
    for a in range(5):
        copies[a].wait()
        for i in range(2):
            rows = pl.ds(8 * i, 8)
            for b in range(5):
                rho, mx, my, en = (u_ref[v, a, b, rows, :] for v in range(4))
                vx, vy, p, inv_rho = velocity_pressure(rho, mx, my, en)
                square = vx * vx + vy * vy
                speed = square * lax.rsqrt(jnp.maximum(square, 1e-37))
                square = ADIABATIC * (p * inv_rho)
                speed = speed + square * lax.rsqrt(square)
                tops[i] = speed if tops[i] is None else jnp.maximum(tops[i], speed)
    top = jnp.max(jnp.maximum(tops[0], tops[1]), axis=0, keepdims=True)
    top_ref[...] = jnp.broadcast_to(top.reshape(1, 1, COLS), top_ref.shape)


def border_kernel(u_ref, raw_ref, cols_ref, even_ref, odd_ref, both_ref):
    raws = []
    for i in range(2):
        rows = pl.ds(8 * i, 8)
        indicator = [[None] * 5 for _ in range(5)]
        for a in range(5):
            for b in range(5):
                cons = [u_ref[v, a, b, rows, :] for v in range(4)]
                indicator[a][b] = cons[0] * velocity_pressure(*cons)[2]
        raws.append(raw_indicator(indicator))
        raw_ref[rows, :] = raws[i]
    pack_borders(
        lambda v, a, b, rows: u_ref[v, a, b, rows, :], raws, cols_ref, even_ref, odd_ref, both_ref
    )


ORDER = ((0, 1, 2, 3), (0, 2, 1, 3))


def node_at(u_ref, work_ref, a, b, normal, load):
    cons = [load(u_ref, (v, a, b)) for v in range(4)]
    return Node(cons, [load(work_ref, (k, a, b)) for k in range(7)], normal)


def row_faces(u_ref, work_ref, faces_ref):
    sublane = sublanes()
    for b in range(5):
        fluxes = []
        for i in range(2):
            rows = pl.ds(8 * i, 8)

            def above(ref, index, i=i):
                if i == 0:
                    return ref[(*index, pl.ds(1, 8), slice(None))]
                return pltpu.roll(ref[(*index, pl.ds(8, 8), slice(None))], 7, 0)

            def here(ref, index, rows=rows):
                return ref[(*index, rows, slice(None))]

            left = node_at(u_ref, work_ref, 4, b, 1, here)
            right = node_at(u_ref, work_ref, 0, b, 1, above)
            fluxes.append(face(left, right))
        for v in range(4):
            first = fluxes[0][v]
            second = jnp.where(sublane == 7, 0.0, fluxes[1][v])
            rolled = pltpu.roll(first, 1, 0)
            faces_ref[0, v, b, 0:8, :] = jnp.where(sublane == 0, 0.0, rolled)
            faces_ref[0, v, b, 8:16, :] = jnp.where(sublane == 0, rolled, pltpu.roll(second, 1, 0))
            faces_ref[1, v, b, 0:8, :] = first
            faces_ref[1, v, b, 8:16, :] = second


def volume_kernel(u_ref, work_ref, high_ref, low_ref, faces_ref):
    row_faces(u_ref, work_ref, faces_ref)
    lane = lanes()

    def chunk(i, carry):
        rows = pl.ds(pl.multiple_of(8 * i, 8), 8)

        def here(ref, index):
            return ref[(*index, rows, slice(None))]

        def after(ref, index):
            return pltpu.roll(here(ref, index), 127, 1)

        for normal in range(2):
            for across in range(5):
                places = [(across, k) if normal == 0 else (k, across) for k in range(5)]
                nodes = [node_at(u_ref, work_ref, a, b, normal, here) for a, b in places]
                if normal == 0:
                    flux = face(nodes[4], node_at(u_ref, work_ref, across, 0, 0, after))
                    upper = [jnp.where(lane == 127, 0.0, x) for x in flux]
                    lower = [pltpu.roll(x, 1, 1) for x in upper]
                else:
                    lower, upper = (
                        [faces_ref[k, v, across, rows, :] for v in range(4)] for k in range(2)
                    )
                sums = line_terms(nodes, lower, upper)
                for ref, terms in zip((high_ref, low_ref), sums):
                    for along, (a, b) in enumerate(places):
                        for k in range(4):
                            v = ORDER[normal][k]
                            term = terms[k][along]
                            if normal == 1:
                                ratio = float(WEIGHTS[b] / WEIGHTS[a])
                                if a not in (b, 4 - b):
                                    term = ratio * term
                                before = ref[v, a, b, rows, :]
                                term = before - term if (a == 4) != (b == 4) else before + term
                            ref[v, a, b, rows, :] = term
        return carry

    lax.fori_loop(0, 2, chunk, 0)


def first_volume_kernel(u_ref, high_ref, low_ref, work_ref, faces_ref):
    def chunk(i, carry):
        rows = pl.ds(pl.multiple_of(8 * i, 8), 8)
        for a in range(5):
            for b in range(5):
                for k, x in enumerate(derived(*(u_ref[v, a, b, rows, :] for v in range(4)))):
                    work_ref[k, a, b, rows, :] = x
        return carry

    lax.fori_loop(0, 2, chunk, 0)
    volume_kernel(u_ref, work_ref, high_ref, low_ref, faces_ref)


def plain(cons, normal):
    return Node(cons, derived(*cons), normal)


def rates(i, high_ref, low_ref, raw_ref, mine, halos, edge_ref):
    my_cols_ref, my_rows_ref = mine
    left_ref, right_ref, below_ref, above_ref = halos
    rows = pl.ds(8 * i, 8)
    lane, sublane = lanes(), sublanes()
    from_left, from_right, own = left_ref[rows, :], right_ref[rows, :], my_cols_ref[rows, :]

    capped = raw_ref[rows, :]
    row_before = below_ref[20:21, :] if i == 0 else raw_ref[7:8, :]
    row_after = above_ref[20:21, :] if i == 1 else raw_ref[8:9, :]
    below = jnp.where(sublane == 0, jnp.broadcast_to(row_before, (8, COLS)), pltpu.roll(capped, 1, 0))
    above = jnp.where(sublane == 7, jnp.broadcast_to(row_after, (8, COLS)), pltpu.roll(capped, 7, 0))
    before = jnp.where(lane == 0, pltpu.roll(from_left, 44, 1), pltpu.roll(capped, 1, 1))
    after = jnp.where(lane == 127, pltpu.roll(from_right, 107, 1), pltpu.roll(capped, 127, 1))
    beside = jnp.maximum(jnp.maximum(below, above), jnp.maximum(before, after))
    blend = jnp.maximum(capped, 0.5 * beside)
    rest = 1.0 - blend
    shares = (0.5 * blend, blend, blend, blend)

    lefts, rights = [], []
    for v in range(4):
        shifted = own if v == 0 else pltpu.roll(own, COLS - 5 * v, 1)
        lefts.append(jnp.where(lane < 64, pltpu.roll(from_left, 64 - 5 * v, 1), shifted))
        rights.append(jnp.where(lane < 64, shifted, pltpu.roll(from_right, 64 - 5 * v, 1)))
    used = jnp.bitwise_and(lane, 63) < 5
    filler = (1.0, 0.0, 0.0, 1.0)
    lefts = [jnp.where(used, x, y) for x, y in zip(lefts, filler)]
    rights = [jnp.where(used, x, y) for x, y in zip(rights, filler)]
    ends = {}
    flux = face(plain(lefts, 0), plain(rights, 0))
    for v in range(4):
        for a in range(5):
            turned = flux[v] if a == 0 else pltpu.roll(flux[v], COLS - a, 1)
            ends[v, a, 0] = jnp.where(lane == 0, turned, 0.0)
            ends[v, a, 4] = jnp.where(lane == 127, pltpu.roll(flux[v], 63 - a, 1), 0.0)
    a = 4 * i
    other_ref = (below_ref, above_ref)[i]
    mine_at = my_rows_ref[i]
    other = [other_ref[5 * v : 5 * v + 5, :] for v in range(4)]
    here = [mine_at[5 * v : 5 * v + 5, :] for v in range(4)]
    sides = (plain(other, 1), plain(here, 1)) if i == 0 else (plain(here, 1), plain(other, 1))
    flux = face(*sides)
    edge = sublane == 7 * i
    for k in range(4):
        v = ORDER[1][k]
        edge_ref[i, 8 * v : 8 * v + 5, :] = flux[k]
        for b in range(5):
            term = jnp.broadcast_to(edge_ref[i, 8 * v + b : 8 * v + b + 1, :], (8, COLS))
            if b not in (0, 4):
                term = float(WEIGHTS[b] / WEIGHTS[a]) * term
            term = jnp.where(edge, term, 0.0)
            same = (a == 4) == (b == 4)
            if (v, a, b) in ends:
                ends[v, a, b] = ends[v, a, b] + term if same else ends[v, a, b] - term
            else:
                ends[v, a, b] = term if a == 0 else -term

    def at(v, a, b):
        x = rest * high_ref[v, a, b, rows, :] + shares[v] * low_ref[v, a, b, rows, :]
        return x - ends[v, a, b] if (v, a, b) in ends else x

    return at


NODES = [(a, b, v) for a in range(5) for b in range(5) for v in range(4)]


def final(v, b):
    return (1.0 if b == 4 else -1.0) * float(PER_WEIGHT[b]) * SCALE[v]


def step_of(tops_ref):
    tops = [tops_ref[k] for k in range(128)]
    while len(tops) > 1:
        tops = [jnp.maximum(x, y) for x, y in zip(tops[::2], tops[1::2])]
    top = jnp.max(tops[0], axis=1, keepdims=True)
    return (COURANT * 2.0 / 9.0) / jnp.broadcast_to(top, (8, COLS))


def first_kernel(
    tops_ref, u_ref, high_ref, low_ref, raw_ref, my_cols_ref, my_even_ref, my_odd_ref, col_even_ref, col_odd_ref, row_even_ref, row_odd_ref,
    step_ref, first_ref, next_raw_ref, next_work_ref, cols_ref, even_ref, odd_ref, both_ref, got_cols_ref, got_rows_ref, my_rows_ref, edge_ref,
):
    step = step_of(tops_ref)
    step_ref[...] = step
    steps = {(v, b): final(v, b) * step for v in (0, 1) for b in range(5)}
    halos = unpack_borders(
        col_even_ref, col_odd_ref, row_even_ref, row_odd_ref, got_cols_ref, got_rows_ref
    )

    mine = own_borders(my_cols_ref, my_even_ref, my_odd_ref, my_rows_ref)

    raws = []
    for i in range(2):
        rows = pl.ds(8 * i, 8)
        at = rates(i, high_ref, low_ref, raw_ref, mine, halos, edge_ref)
        for a, b, v in NODES:
            first_ref[v, a, b, rows, :] = u_ref[v, a, b, rows, :] + steps[min(v, 1), b] * at(v, a, b)
        indicator = [[None] * 5 for _ in range(5)]
        for a in range(5):
            for b in range(5):
                cons = [first_ref[v, a, b, rows, :] for v in range(4)]
                values = derived(*cons)
                for k, x in enumerate(values):
                    next_work_ref[k, a, b, rows, :] = x
                indicator[a][b] = cons[0] * values[2]
        raws.append(raw_indicator(indicator))
        next_raw_ref[rows, :] = raws[i]
    pack_borders(
        lambda v, a, b, rows: first_ref[v, a, b, rows, :],
        raws, cols_ref, even_ref, odd_ref, both_ref,
    )


def last_kernel(
    step_ref, u_ref, first_ref, high_ref, low_ref, raw_ref, my_cols_ref, my_even_ref, my_odd_ref, col_even_ref, col_odd_ref, row_even_ref, row_odd_ref,
    advanced_ref, tendency_ref, got_cols_ref, got_rows_ref, my_rows_ref, edge_ref, advanced_vmem, tendency_vmem, sent,
):
    half = 0.5 * step_ref[...]
    halos = unpack_borders(
        col_even_ref, col_odd_ref, row_even_ref, row_odd_ref, got_cols_ref, got_rows_ref
    )
    mine = own_borders(my_cols_ref, my_even_ref, my_odd_ref, my_rows_ref)
    copies = []

    ats = [rates(i, high_ref, low_ref, raw_ref, mine, halos, edge_ref) for i in range(2)]
    for a in range(5):
        for i in range(2):
            rows = pl.ds(8 * i, 8)
            for b in range(5):
                for v in range(4):
                    rate = final(v, b) * ats[i](v, a, b)
                    tendency_vmem[v, a, b, rows, :] = rate
                    states = u_ref[v, a, b, rows, :] + first_ref[v, a, b, rows, :]
                    advanced_vmem[v, a, b, rows, :] = 0.5 * states + half * rate
        for kept, out in ((advanced_vmem, advanced_ref), (tendency_vmem, tendency_ref)):
            copies.append(
                pltpu.make_async_copy(kept.at[:, a], out.at[:, a], sent.at[len(copies)])
            )
            copies[-1].start()
    for copy in copies:
        copy.wait()


FIELD = jax.ShapeDtypeStruct((4, 5, 5, ROWS, COLS), F32)
RAW = jax.ShapeDtypeStruct((ROWS, COLS), F32)
ROW = jax.ShapeDtypeStruct((24, COLS), F32)
WORK = jax.ShapeDtypeStruct((7, 5, 5, ROWS, COLS), F32)
TILE = jax.ShapeDtypeStruct((8, COLS), F32)
TOPS = jax.ShapeDtypeStruct((128, 1, COLS), F32)


def call(kernel, outs, scratch=(), hbm_in=False, hbm_out=False):
    here, there = pl.BlockSpec(memory_space=pltpu.VMEM), pl.BlockSpec(memory_space=pltpu.HBM)

    def run(*args):
        space = pltpu.HBM if hbm_in else pltpu.VMEM
        args = [pltpu.with_memory_space_constraint(x, space) for x in args]
        return pl.pallas_call(
            kernel,
            out_shape=tuple(o if hbm_out else pltpu.VMEM(o.shape, o.dtype) for o in outs),
            in_specs=[there if hbm_in else here for _ in args],
            out_specs=tuple(there if hbm_out else here for _ in outs),
            scratch_shapes=list(scratch),
            compiler_params=pltpu.CompilerParams(vmem_limit_bytes=16 << 20),
        )(*args)

    return run


BOTH = pltpu.VMEM((2, 24, COLS), F32)
GOT = (
    pltpu.VMEM((2, ROWS, COLS), F32),
    pltpu.VMEM((2, 24, COLS), F32),
    pltpu.VMEM((2, 24, COLS), F32),
    pltpu.VMEM((2, 32, COLS), F32),
)
FACES = pltpu.VMEM((2, 4, 5, ROWS, COLS), F32)


SWAPS = (("col_odd", 0, GX, 1), ("col_even", 0, GX, 0), ("row_odd", 2, GY, 1), ("row_even", 1, GY, 0))


def borders(cols, even, odd):
    def swap(x, axis, second):
        count = lax.axis_size(axis)
        pairs = [(i, (((i + second) ^ 1) - second) % count) for i in range(count)]
        return lax.ppermute(x, axis, pairs)

    got = {}
    for name, sent, axis, second in SWAPS:
        got[name] = swap((cols, even, odd)[sent], axis, second)
    return got["col_even"], got["col_odd"], got["row_even"], got["row_odd"]


def local(state):
    top, state = call(
        start_kernel, (TOPS, FIELD), (pltpu.SemaphoreType.DMA((5,)),), hbm_in=True
    )(state)
    tops = lax.all_to_all(top, ALL, 0, 0, tiled=True)
    raw, *mine = call(border_kernel, (RAW, RAW, ROW, ROW), (BOTH,))(state)
    halos = borders(*mine)
    work = pltpu.VMEM(WORK.shape, F32)
    high, low = call(first_volume_kernel, (FIELD, FIELD), (work, FACES))(state)
    step, first, raw, work, *next_mine = call(
        first_kernel, (TILE, FIELD, RAW, WORK, RAW, ROW, ROW), (BOTH, *GOT)
    )(tops, state, high, low, raw, *mine, *halos)
    halos = borders(*next_mine)
    high, low = call(volume_kernel, (FIELD, FIELD), (FACES,))(first, work)
    kept = pltpu.VMEM(FIELD.shape, F32)
    return call(
        last_kernel, (FIELD, FIELD), (*GOT, kept, kept, pltpu.SemaphoreType.DMA((10,))), hbm_out=True
    )(step, state, first, high, low, raw, *next_mine, *halos)


def solution(mesh):
    torus = Mesh(mesh.devices.reshape(4, 4, 4, 2), ALL)
    return jax.shard_map(
        local,
        mesh=torus,
        in_specs=(P(None, None, None, GY, GX),),
        out_specs=(P(None, None, None, GY, GX), P(None, None, None, GY, GX)),
        check_vma=False,
    )
```

```python
import math

import jax
import jax.numpy as jnp
import numpy as np
from jax import lax
from jax.experimental import pallas as pl
from jax.experimental.pallas import tpu as pltpu
from jax.sharding import Mesh
from jax.sharding import PartitionSpec as P


GX = ("gx_0", "gx_1")
GY = ("gy_0", "gy_1")
ALL = ("gx_0", "gx_1", "gy_0", "gy_1")


ADIABATIC = 1.4
COURANT = 0.2
ALPHA_MAX = 0.5
ROWS = 16
COLS = 128
F32 = jnp.float32


def tables():
    lobatto = np.array([-1.0, -math.sqrt(3.0 / 7.0), 0.0, math.sqrt(3.0 / 7.0), 1.0])
    weights = np.array([0.1, 49.0 / 90.0, 32.0 / 45.0, 49.0 / 90.0, 0.1])
    identity = np.eye(5)
    distance = lobatto[:, None] - lobatto[None, :] + identity
    barycentric = 1.0 / np.prod(distance, axis=1)
    derivative = (1.0 - identity) * (barycentric[None, :] / barycentric[:, None]) / distance
    derivative = derivative - identity * derivative.sum(axis=1)[:, None]
    legendre = np.zeros((5, 5))
    legendre[:, 0] = 1.0
    legendre[:, 1] = lobatto
    for degree in range(2, 5):
        legendre[:, degree] = (
            (2 * degree - 1) * lobatto * legendre[:, degree - 1]
            - (degree - 1) * legendre[:, degree - 2]
        ) / degree
    norms = np.array([2.0, 2.0 / 3.0, 2.0 / 5.0, 2.0 / 7.0, 0.5])
    inverse = (legendre * weights[:, None]).T / norms[:, None]
    return derivative, weights, inverse


DERIVATIVE, WEIGHTS, INVERSE = tables()
SKEW = WEIGHTS[:, None] * DERIVATIVE
PER_WEIGHT = 1.0 / WEIGHTS
SCALE = (1.0, 0.5, 0.5, 0.5)
LN2 = math.log(2.0)


LN2 = math.log(2.0)
NEAR = math.log2(1.01 / 0.99)


def velocity_pressure(rho, mx, my, en):
    inv_rho = 1.0 / rho
    vx = mx * inv_rho
    vy = my * inv_rho
    pressure = 0.4 * en - 0.2 * (mx * vx + my * vy)
    return vx, vy, pressure, inv_rho


def sound(theta):
    square = (ADIABATIC / (5.0 * LN2)) * theta
    return square * lax.rsqrt(square)


def derived(rho, mx, my, en):
    vx, vy, p, inv_rho = velocity_pressure(rho, mx, my, en)
    theta = (5.0 * LN2) * (p * inv_rho)
    return vx, vy, p, rho * ((0.2 / LN2) / p), theta, inv_rho, sound(theta)


class Node:
    def __init__(self, cons, values, normal):
        rho, mx, my, en = cons
        vx, vy, p, beta, theta, inv_rho, c = values
        self.rho, self.en, self.p = rho, en, p
        self.beta, self.theta, self.inv_rho = beta, theta, inv_rho
        self.vn, self.vt, self.mn, self.mt = (vx, vy, mx, my) if normal == 0 else (vy, vx, my, mx)
        self.speed = jnp.abs(self.vn) + c
        self.cons = (rho, self.mn, self.mt, en)


def series(f):
    c = [2.0 / (k * LN2) for k in (1, 3, 5, 7)]
    return c[0] + f * (c[1] + f * (c[2] + f * c[3]))


def pair(left, right, q):
    s = left.rho + right.rho
    d = right.rho - left.rho
    logged = lax.log2(right.rho * left.inv_rho)
    near = jnp.abs(logged) < NEAR
    t = d * (1.0 / jnp.where(near, s, logged))
    mean = jnp.where(near, s * (1.0 / series(t * t)), t)
    s = left.beta + right.beta
    d = right.beta - left.beta
    logged = lax.log2(right.beta * left.theta)
    near = jnp.abs(logged) < NEAR
    r = 1.0 / jnp.where(near, s, d)
    t = d * r
    warm = jnp.where(near, series(t * t), logged) * r
    vn = left.vn + right.vn
    vt = left.vt + right.vt
    ps = left.p + right.p
    cross = left.p * right.vn + right.p * left.vn
    if q != 0.5:
        ps = ps * (2.0 * q)
        cross = cross * (2.0 * q)
    mass = (mean * vn) * (q / LN2)
    along = mass * vn + ps
    across = mass * vt
    dot = left.vn * right.vn + left.vt * right.vt
    energy = mass * (dot + warm) + cross
    return mass, along, across, energy


def line_terms(nodes, lower, upper):
    high = [[None] * 5 for _ in range(4)]
    for j in range(4, 0, -1):
        for i in range(j):
            flux = pair(nodes[i], nodes[j], float(SKEW[i, j]))
            for v in range(4):
                high[v][i] = flux[v] if high[v][i] is None else high[v][i] + flux[v]
                if j == 4:
                    high[v][4] = flux[v] if high[v][4] is None else high[v][4] + flux[v]
                else:
                    high[v][j] = high[v][j] - flux[v]
    own = []
    for node in nodes:
        flow = node.mn * node.vn + node.p
        own.append((node.mn, flow, node.mn * node.vt, node.vn * (node.en + node.p)))
    low = [[None] * 5 for _ in range(4)]
    for v in range(4):
        before = None
        for i in range(4):
            spread = jnp.maximum(nodes[i].speed, nodes[i + 1].speed)
            jump = nodes[i + 1].cons[v] - nodes[i].cons[v]
            inner = own[i][v] + own[i + 1][v] - spread * jump
            low[v][i] = inner if before is None else inner - before
            before = inner
        low[v][4] = before
        for i, flux in ((0, lower[v]), (4, upper[v])):
            high[v][i] = high[v][i] - flux
            low[v][i] = low[v][i] - (flux + flux if v == 0 else flux)
    return high, low


def face(left, right):
    flux = pair(left, right, 0.5)
    fastest = jnp.maximum(left.speed, right.speed)
    out = []
    for v in range(4):
        jump = fastest * (right.cons[v] - left.cons[v])
        out.append(flux[v] - (0.5 * jump if v == 0 else jump))
    return out


def transform(values):
    s0, s1 = values[0] + values[4], values[1] + values[3]
    d0, d1 = values[0] - values[4], values[1] - values[3]
    out = []
    for k in range(5):
        c = [float(x) for x in INVERSE[k]]
        if k % 2 == 0:
            out.append(c[0] * s0 + c[1] * s1 + c[2] * values[2])
        else:
            out.append(c[0] * d0 + c[1] * d1)
    return out


def raw_indicator(indicator):
    along = [transform(indicator[a]) for a in range(5)]
    modal = [transform([along[a][l] for a in range(5)]) for l in range(5)]
    levels = [None] * 5
    for l in range(5):
        for k in range(5):
            square = modal[l][k] * modal[l][k]
            level = max(k, l)
            levels[level] = square if levels[level] is None else levels[level] + square
    lower = levels[0] + levels[1] + levels[2] + levels[3]
    total = lower + levels[4]
    energy = jnp.maximum(levels[4] / total, levels[3] / lower)
    threshold = 0.5 * 10.0 ** (-1.8 * 5.0**0.25)
    sharpness = math.log((1.0 - 0.0001) / 0.0001)
    sigmoid = 1.0 / (1.0 + jnp.exp(-sharpness / threshold * (energy - threshold)))
    return jnp.minimum(sigmoid, ALPHA_MAX)


def lanes():
    return lax.broadcasted_iota(jnp.int32, (8, COLS), 1)


def sublanes():
    return lax.broadcasted_iota(jnp.int32, (8, COLS), 0)


def odd_column():
    return lax.rem(lax.axis_index("gx_1"), 2)


def odd_row():
    return lax.axis_index("gy_1")


def pack_borders(get, raws, cols_ref, even_ref, odd_ref, both_ref):
    up_ref, down_ref = both_ref.at[0], both_ref.at[1]
    lane = lanes()
    for i in range(2):
        packed = jnp.zeros((8, COLS), F32)
        for v in range(4):
            for a in range(5):
                j = v * 5 + a
                first = get(v, a, 0, pl.ds(8 * i, 8))
                last = get(v, a, 4, pl.ds(8 * i, 8))
                packed = jnp.where(lane == j, first if j == 0 else pltpu.roll(first, j, 1), packed)
                packed = jnp.where(lane == 64 + j, pltpu.roll(last, 65 + j, 1), packed)
        packed = jnp.where(lane == 20, pltpu.roll(raws[i], 20, 1), packed)
        packed = jnp.where(lane == 84, pltpu.roll(raws[i], 85, 1), packed)
        cols_ref[pl.ds(8 * i, 8), :] = packed
    for v in range(4):
        for b in range(5):
            j = v * 5 + b
            up_ref[j : j + 1, :] = get(v, 4, b, pl.ds(15, 1))
            down_ref[j : j + 1, :] = get(v, 0, b, pl.ds(0, 1))
    up_ref[20:21, :] = raws[1][7:8, :]
    down_ref[20:21, :] = raws[0][0:1, :]
    zeros = jnp.zeros((3, COLS), F32)
    up_ref[21:24, :] = zeros
    down_ref[21:24, :] = zeros
    odd = odd_row()
    even_ref[...] = both_ref[odd]
    odd_ref[...] = both_ref[1 - odd]


def unpack_borders(col_even_ref, col_odd_ref, row_even_ref, row_odd_ref, cols_ref, rows_ref):
    cols_ref[0] = col_even_ref[...]
    cols_ref[1] = col_odd_ref[...]
    rows_ref[0] = row_even_ref[...]
    rows_ref[1] = row_odd_ref[...]
    odd = odd_column()
    left, right = cols_ref.at[1 - odd], cols_ref.at[odd]
    odd = odd_row()
    below, above = rows_ref.at[1 - odd], rows_ref.at[odd]
    return left, right, below, above


def own_borders(cols_ref, even_ref, odd_ref, rows_ref):
    rows_ref[0] = even_ref[...]
    rows_ref[1] = odd_ref[...]
    odd = odd_row()
    return cols_ref, (rows_ref.at[1 - odd], rows_ref.at[odd])


def start_kernel(
    state_ref, top_ref, u_ref, raw_ref, cols_ref, even_ref, odd_ref, arrived, top_vmem, sent, both_ref
):
    copies = [
        pltpu.make_async_copy(state_ref.at[:, a], u_ref.at[:, a], arrived.at[a]) for a in range(5)
    ]
    for copy in copies:
        copy.start()
    tops = [None, None]
    indicators = [[[None] * 5 for _ in range(5)] for _ in range(2)]
    for a in range(5):
        copies[a].wait()
        for i in range(2):
            rows = pl.ds(8 * i, 8)
            for b in range(5):
                rho, mx, my, en = (u_ref[v, a, b, rows, :] for v in range(4))
                vx, vy, p, inv_rho = velocity_pressure(rho, mx, my, en)
                indicators[i][a][b] = rho * p
                square = vx * vx + vy * vy
                speed = square * lax.rsqrt(jnp.maximum(square, 1e-37))
                square = ADIABATIC * (p * inv_rho)
                speed = speed + square * lax.rsqrt(square)
                tops[i] = speed if tops[i] is None else jnp.maximum(tops[i], speed)
    top = jnp.max(jnp.maximum(tops[0], tops[1]), axis=0, keepdims=True)
    top_vmem[...] = jnp.broadcast_to(top.reshape(1, 1, COLS), top_vmem.shape)
    copy = pltpu.make_async_copy(top_vmem, top_ref, sent)
    copy.start()
    raws = []
    for i in range(2):
        raws.append(raw_indicator(indicators[i]))
        raw_ref[pl.ds(8 * i, 8), :] = raws[i]
    pack_borders(
        lambda v, a, b, rows: u_ref[v, a, b, rows, :], raws, cols_ref, even_ref, odd_ref, both_ref
    )
    copy.wait()


ORDER = ((0, 1, 2, 3), (0, 2, 1, 3))


def node_at(u_ref, work_ref, a, b, normal, load):
    cons = [load(u_ref, (v, a, b)) for v in range(4)]
    return Node(cons, [load(work_ref, (k, a, b)) for k in range(7)], normal)


def row_faces(u_ref, work_ref, faces_ref):
    sublane = sublanes()
    for b in range(5):
        fluxes = []
        for i in range(2):
            rows = pl.ds(8 * i, 8)

            def above(ref, index, i=i):
                if i == 0:
                    return ref[(*index, pl.ds(1, 8), slice(None))]
                return pltpu.roll(ref[(*index, pl.ds(8, 8), slice(None))], 7, 0)

            def here(ref, index, rows=rows):
                return ref[(*index, rows, slice(None))]

            left = node_at(u_ref, work_ref, 4, b, 1, here)
            right = node_at(u_ref, work_ref, 0, b, 1, above)
            fluxes.append(face(left, right))
        for v in range(4):
            first = fluxes[0][v]
            second = jnp.where(sublane == 7, 0.0, fluxes[1][v])
            rolled = pltpu.roll(first, 1, 0)
            faces_ref[0, v, b, 0:8, :] = jnp.where(sublane == 0, 0.0, rolled)
            faces_ref[0, v, b, 8:16, :] = jnp.where(sublane == 0, rolled, pltpu.roll(second, 1, 0))
            faces_ref[1, v, b, 0:8, :] = first
            faces_ref[1, v, b, 8:16, :] = second


def volume_kernel(u_ref, work_ref, high_ref, low_ref, faces_ref):
    row_faces(u_ref, work_ref, faces_ref)
    lane = lanes()

    def chunk(i, carry):
        rows = pl.ds(pl.multiple_of(8 * i, 8), 8)

        def here(ref, index):
            return ref[(*index, rows, slice(None))]

        def after(ref, index):
            return pltpu.roll(here(ref, index), 127, 1)

        for normal in range(2):
            for across in range(5):
                places = [(across, k) if normal == 0 else (k, across) for k in range(5)]
                nodes = [node_at(u_ref, work_ref, a, b, normal, here) for a, b in places]
                if normal == 0:
                    flux = face(nodes[4], node_at(u_ref, work_ref, across, 0, 0, after))
                    upper = [jnp.where(lane == 127, 0.0, x) for x in flux]
                    lower = [pltpu.roll(x, 1, 1) for x in upper]
                else:
                    lower, upper = (
                        [faces_ref[k, v, across, rows, :] for v in range(4)] for k in range(2)
                    )
                sums = line_terms(nodes, lower, upper)
                for ref, terms in zip((high_ref, low_ref), sums):
                    for along, (a, b) in enumerate(places):
                        for k in range(4):
                            v = ORDER[normal][k]
                            term = terms[k][along]
                            if normal == 1:
                                ratio = float(WEIGHTS[b] / WEIGHTS[a])
                                if a not in (b, 4 - b):
                                    term = ratio * term
                                before = ref[v, a, b, rows, :]
                                term = before - term if (a == 4) != (b == 4) else before + term
                            ref[v, a, b, rows, :] = term
        return carry

    lax.fori_loop(0, 2, chunk, 0)


def first_volume_kernel(u_ref, high_ref, low_ref, work_ref, faces_ref):
    def chunk(i, carry):
        rows = pl.ds(pl.multiple_of(8 * i, 8), 8)
        for a in range(5):
            for b in range(5):
                for k, x in enumerate(derived(*(u_ref[v, a, b, rows, :] for v in range(4)))):
                    work_ref[k, a, b, rows, :] = x
        return carry

    lax.fori_loop(0, 2, chunk, 0)
    volume_kernel(u_ref, work_ref, high_ref, low_ref, faces_ref)


def plain(cons, normal):
    return Node(cons, derived(*cons), normal)


def rates(i, high_ref, low_ref, raw_ref, mine, halos, edge_ref):
    my_cols_ref, my_rows_ref = mine
    left_ref, right_ref, below_ref, above_ref = halos
    rows = pl.ds(8 * i, 8)
    lane, sublane = lanes(), sublanes()
    from_left, from_right, own = left_ref[rows, :], right_ref[rows, :], my_cols_ref[rows, :]

    capped = raw_ref[rows, :]
    row_before = below_ref[20:21, :] if i == 0 else raw_ref[7:8, :]
    row_after = above_ref[20:21, :] if i == 1 else raw_ref[8:9, :]
    below = jnp.where(sublane == 0, jnp.broadcast_to(row_before, (8, COLS)), pltpu.roll(capped, 1, 0))
    above = jnp.where(sublane == 7, jnp.broadcast_to(row_after, (8, COLS)), pltpu.roll(capped, 7, 0))
    before = jnp.where(lane == 0, pltpu.roll(from_left, 44, 1), pltpu.roll(capped, 1, 1))
    after = jnp.where(lane == 127, pltpu.roll(from_right, 107, 1), pltpu.roll(capped, 127, 1))
    beside = jnp.maximum(jnp.maximum(below, above), jnp.maximum(before, after))
    blend = jnp.maximum(capped, 0.5 * beside)
    rest = 1.0 - blend
    shares = (0.5 * blend, blend, blend, blend)

    lefts, rights = [], []
    for v in range(4):
        shifted = own if v == 0 else pltpu.roll(own, COLS - 5 * v, 1)
        lefts.append(jnp.where(lane < 64, pltpu.roll(from_left, 64 - 5 * v, 1), shifted))
        rights.append(jnp.where(lane < 64, shifted, pltpu.roll(from_right, 64 - 5 * v, 1)))
    used = jnp.bitwise_and(lane, 63) < 5
    filler = (1.0, 0.0, 0.0, 1.0)
    lefts = [jnp.where(used, x, y) for x, y in zip(lefts, filler)]
    rights = [jnp.where(used, x, y) for x, y in zip(rights, filler)]
    ends = {}
    flux = face(plain(lefts, 0), plain(rights, 0))
    for v in range(4):
        for a in range(5):
            turned = flux[v] if a == 0 else pltpu.roll(flux[v], COLS - a, 1)
            ends[v, a, 0] = jnp.where(lane == 0, turned, 0.0)
            ends[v, a, 4] = jnp.where(lane == 127, pltpu.roll(flux[v], 63 - a, 1), 0.0)
    a = 4 * i
    other_ref = (below_ref, above_ref)[i]
    mine_at = my_rows_ref[i]
    other = [other_ref[5 * v : 5 * v + 5, :] for v in range(4)]
    here = [mine_at[5 * v : 5 * v + 5, :] for v in range(4)]
    sides = (plain(other, 1), plain(here, 1)) if i == 0 else (plain(here, 1), plain(other, 1))
    flux = face(*sides)
    edge = sublane == 7 * i
    for k in range(4):
        v = ORDER[1][k]
        edge_ref[i, 8 * v : 8 * v + 5, :] = flux[k]
        for b in range(5):
            term = jnp.broadcast_to(edge_ref[i, 8 * v + b : 8 * v + b + 1, :], (8, COLS))
            if b not in (0, 4):
                term = float(WEIGHTS[b] / WEIGHTS[a]) * term
            term = jnp.where(edge, term, 0.0)
            same = (a == 4) == (b == 4)
            if (v, a, b) in ends:
                ends[v, a, b] = ends[v, a, b] + term if same else ends[v, a, b] - term
            else:
                ends[v, a, b] = term if a == 0 else -term

    def at(v, a, b):
        x = rest * high_ref[v, a, b, rows, :] + shares[v] * low_ref[v, a, b, rows, :]
        return x - ends[v, a, b] if (v, a, b) in ends else x

    return at


NODES = [(a, b, v) for a in range(5) for b in range(5) for v in range(4)]


def final(v, b):
    return (1.0 if b == 4 else -1.0) * float(PER_WEIGHT[b]) * SCALE[v]


def step_of(tops_ref):
    tops = [tops_ref[k] for k in range(128)]
    while len(tops) > 1:
        tops = [jnp.maximum(x, y) for x, y in zip(tops[::2], tops[1::2])]
    top = jnp.max(tops[0], axis=1, keepdims=True)
    return (COURANT * 2.0 / 9.0) / jnp.broadcast_to(top, (8, COLS))


def rate_kernel(
    high_ref, low_ref, raw_ref, my_cols_ref, my_even_ref, my_odd_ref, col_even_ref, col_odd_ref, row_even_ref, row_odd_ref,
    rate_ref, got_cols_ref, got_rows_ref, my_rows_ref, edge_ref,
):
    halos = unpack_borders(
        col_even_ref, col_odd_ref, row_even_ref, row_odd_ref, got_cols_ref, got_rows_ref
    )
    mine = own_borders(my_cols_ref, my_even_ref, my_odd_ref, my_rows_ref)
    for i in range(2):
        at = rates(i, high_ref, low_ref, raw_ref, mine, halos, edge_ref)
        for a, b, v in NODES:
            rate_ref[v, a, b, pl.ds(8 * i, 8), :] = at(v, a, b)


def first_kernel(
    tops_ref, u_ref, rate_ref,
    step_ref, first_ref, next_raw_ref, next_work_ref, cols_ref, even_ref, odd_ref, both_ref,
):
    step = step_of(tops_ref)
    step_ref[...] = step
    steps = {(v, b): final(v, b) * step for v in (0, 1) for b in range(5)}
    raws = []
    for i in range(2):
        rows = pl.ds(8 * i, 8)
        indicator = [[None] * 5 for _ in range(5)]
        for a in range(5):
            for b in range(5):
                cons = []
                for v in range(4):
                    change = steps[min(v, 1), b] * rate_ref[v, a, b, rows, :]
                    cons.append(u_ref[v, a, b, rows, :] + change)
                    first_ref[v, a, b, rows, :] = cons[v]
                values = derived(*cons)
                for k, x in enumerate(values):
                    next_work_ref[k, a, b, rows, :] = x
                indicator[a][b] = cons[0] * values[2]
        raws.append(raw_indicator(indicator))
        next_raw_ref[rows, :] = raws[i]
    pack_borders(
        lambda v, a, b, rows: first_ref[v, a, b, rows, :],
        raws, cols_ref, even_ref, odd_ref, both_ref,
    )


def last_kernel(
    step_ref, u_ref, first_ref, high_ref, low_ref, raw_ref, my_cols_ref, my_even_ref, my_odd_ref, col_even_ref, col_odd_ref, row_even_ref, row_odd_ref,
    advanced_ref, tendency_ref, got_cols_ref, got_rows_ref, my_rows_ref, edge_ref, advanced_vmem, tendency_vmem, sent,
):
    half = 0.5 * step_ref[...]
    halos = unpack_borders(
        col_even_ref, col_odd_ref, row_even_ref, row_odd_ref, got_cols_ref, got_rows_ref
    )
    mine = own_borders(my_cols_ref, my_even_ref, my_odd_ref, my_rows_ref)
    copies = []

    ats = [rates(i, high_ref, low_ref, raw_ref, mine, halos, edge_ref) for i in range(2)]
    for a in range(5):
        for i in range(2):
            rows = pl.ds(8 * i, 8)
            for b in range(5):
                for v in range(4):
                    rate = final(v, b) * ats[i](v, a, b)
                    tendency_vmem[v, a, b, rows, :] = rate
                    states = u_ref[v, a, b, rows, :] + first_ref[v, a, b, rows, :]
                    advanced_vmem[v, a, b, rows, :] = 0.5 * states + half * rate
        for kept, out in ((advanced_vmem, advanced_ref), (tendency_vmem, tendency_ref)):
            copies.append(
                pltpu.make_async_copy(kept.at[:, a], out.at[:, a], sent.at[len(copies)])
            )
            copies[-1].start()
    for copy in copies:
        copy.wait()


FIELD = jax.ShapeDtypeStruct((4, 5, 5, ROWS, COLS), F32)
RAW = jax.ShapeDtypeStruct((ROWS, COLS), F32)
ROW = jax.ShapeDtypeStruct((24, COLS), F32)
WORK = jax.ShapeDtypeStruct((7, 5, 5, ROWS, COLS), F32)
TILE = jax.ShapeDtypeStruct((8, COLS), F32)
TOPS = jax.ShapeDtypeStruct((128, 1, COLS), F32)


def call(kernel, outs, scratch=(), hbm_in=False, hbm_out=0):
    here, there = pl.BlockSpec(memory_space=pltpu.VMEM), pl.BlockSpec(memory_space=pltpu.HBM)

    def run(*args):
        space = pltpu.HBM if hbm_in else pltpu.VMEM
        args = [pltpu.with_memory_space_constraint(x, space) for x in args]
        return pl.pallas_call(
            kernel,
            out_shape=tuple(
                o if k < hbm_out else pltpu.VMEM(o.shape, o.dtype) for k, o in enumerate(outs)
            ),
            in_specs=[there if hbm_in else here for _ in args],
            out_specs=tuple(there if k < hbm_out else here for k, _ in enumerate(outs)),
            scratch_shapes=list(scratch),
            compiler_params=pltpu.CompilerParams(vmem_limit_bytes=16 << 20),
        )(*args)

    return run


BOTH = pltpu.VMEM((2, 24, COLS), F32)
GOT = (
    pltpu.VMEM((2, ROWS, COLS), F32),
    pltpu.VMEM((2, 24, COLS), F32),
    pltpu.VMEM((2, 24, COLS), F32),
    pltpu.VMEM((2, 32, COLS), F32),
)
FACES = pltpu.VMEM((2, 4, 5, ROWS, COLS), F32)


SWAPS = (("col_odd", 0, GX, 1), ("col_even", 0, GX, 0), ("row_odd", 2, GY, 1), ("row_even", 1, GY, 0))


def borders(cols, even, odd):
    def swap(x, axis, second):
        count = lax.axis_size(axis)
        pairs = [(i, (((i + second) ^ 1) - second) % count) for i in range(count)]
        return lax.ppermute(x, axis, pairs)

    got = {}
    for name, sent, axis, second in SWAPS:
        got[name] = swap((cols, even, odd)[sent], axis, second)
    return got["col_even"], got["col_odd"], got["row_even"], got["row_odd"]


def local(state):
    scratch = (
        pltpu.SemaphoreType.DMA((5,)),
        pltpu.VMEM(TOPS.shape, F32),
        pltpu.SemaphoreType.DMA,
        BOTH,
    )
    top, state, raw, *mine = call(
        start_kernel, (TOPS, FIELD, RAW, RAW, ROW, ROW), scratch, hbm_in=True, hbm_out=1
    )(state)
    work = pltpu.VMEM(WORK.shape, F32)
    tops = lax.all_to_all(top, ALL, 0, 0, tiled=True)
    halos = borders(*mine)
    high, low = call(first_volume_kernel, (FIELD, FIELD), (work, FACES))(state)
    (rate,) = call(rate_kernel, (FIELD,), GOT)(high, low, raw, *mine, *halos)
    step, first, raw, work, *next_mine = call(
        first_kernel, (TILE, FIELD, RAW, WORK, RAW, ROW, ROW), (BOTH,)
    )(tops, state, rate)
    halos = borders(*next_mine)
    high, low = call(volume_kernel, (FIELD, FIELD), (FACES,))(first, work)
    kept = pltpu.VMEM(FIELD.shape, F32)
    return call(
        last_kernel, (FIELD, FIELD), (*GOT, kept, kept, pltpu.SemaphoreType.DMA((10,))), hbm_out=2
    )(step, state, first, high, low, raw, *next_mine, *halos)


def solution(mesh):
    torus = Mesh(mesh.devices.reshape(4, 4, 4, 2), ALL)
    return jax.shard_map(
        local,
        mesh=torus,
        in_specs=(P(None, None, None, GY, GX),),
        out_specs=(P(None, None, None, GY, GX), P(None, None, None, GY, GX)),
        check_vma=False,
    )
```
